256 devices in a mesh: seq: 64 (over z, y, core), head: 4 (over x).
Axes of the slice: x: 4, y: 4, z: 8, core: 2. Of those that a mesh axis runs over, the one named last changes fastest.
Arguments:
- queries: bfloat16 [16384, 4096], P('seq', 'head'), may hold values from -5 to 5
- keys: bfloat16 [16384, 4096], P('seq', 'head'), may hold values from -5 to 5
- values: bfloat16 [16384, 4096], P('seq', 'head'), may hold values from -6 to 6
- beta: float32 [32], P('head'), may hold values from -2 to 2
- w_out: bfloat16 [4096, 4096], P('head'), may hold values from -0.09375 to 0.09375
Outputs:
- mixed: bfloat16 [16384, 4096], P('seq', 'head')
The draws below stay inside these ranges and needn't reach their ends.
All inputs are finite; a program needn't handle non-finite values.
Results may differ from the reference program's by a relative error of at most 0.0069.
Values may be sent and summed in bfloat16 or wider, within the bound.
A program may use at most 192 MiB of HBM per device.

```python
import jax
import jax.numpy as jnp
from jax import lax

D = 4096
HEADS = 32
HD = 128
SEG = 2048
TOKENS = 16384


def draw_queries(key, part):
    own_key = jax.random.fold_in(key, 11)
    extent = (TOKENS, HEADS * HD)
    base = jnp.clip(0.7 * jax.random.normal(own_key, extent, jnp.float32), -5.0, 5.0)
    return base.astype(jnp.bfloat16)


def draw_keys(key, part):
    own_key = jax.random.fold_in(key, 12)
    extent = (TOKENS, HEADS * HD)
    position = jnp.arange(TOKENS)
    rising = (3.0 * position.astype(jnp.float32) / TOKENS)[:, None]
    base = jnp.clip(jax.random.normal(own_key, extent, jnp.float32) + rising, -5.0, 5.0)
    return base.astype(jnp.bfloat16)


def draw_values(key, part):
    own_key = jax.random.fold_in(key, 13)
    extent = (TOKENS, HEADS * HD)
    segments = TOKENS // SEG
    offsets = jax.random.normal(jax.random.fold_in(key, 14), (segments, HEADS * HD), jnp.float32)
    noise = jax.random.normal(own_key, extent, jnp.float32)
    spread = jnp.repeat(offsets, SEG, axis=0)
    return jnp.clip(0.8 * noise + 0.8 * spread, -6.0, 6.0).astype(jnp.bfloat16)


def steps_of(key, shape, split, low, largest):
    loudness = 1.0
    for dim, shards_of in split:
        draws = jax.random.uniform(jax.random.fold_in(jax.random.fold_in(key, 6), dim), (shards_of,), jnp.float32, low / len(split), largest / len(split))
        loudness = loudness * jnp.repeat(jnp.exp(draws), shape[dim] // shards_of).reshape((-1,) + (1,) * (len(shape) - 1 - dim))
    return loudness


def gaussian(key, shape, scale, bound, pieces=(), held_as=jnp.bfloat16):
    values = scale * jax.random.normal(key, shape, jnp.float32)
    if pieces:
        values = values * steps_of(key, shape, pieces, -0.22, 0.18)
    return jnp.clip(values, -bound, bound).astype(held_as)


def setup_inputs(seed: int = 0) -> dict:
    streams_of = jax.random.split(jax.random.key(seed), 6)
    queries = draw_queries(jax.random.fold_in(streams_of[5], 71), 0)
    keys = draw_keys(jax.random.fold_in(streams_of[5], 71), 0)
    values = draw_values(jax.random.fold_in(streams_of[5], 71), 0)
    beta = jnp.clip(jax.random.uniform(streams_of[3], (HEADS,), jnp.float32, -2.0, 2.0) * steps_of(streams_of[3], (HEADS,), ((0, 4),), -0.4, 0.0), -2.0, 2.0)
    w_out = gaussian(streams_of[4], (HEADS * HD, D), (HEADS * HD) ** -0.5, 0.09375, ((0, 4),))
    return dict(queries=queries, keys=keys, values=values, beta=beta, w_out=w_out)


def elu_plus(inputs):
    return jnp.where(inputs > 0, inputs + 1.0, jnp.exp(jnp.minimum(inputs, 0.0)))


def window_head(packed):
    query_head, key_head, value_head, first_flag = packed
    scores = jnp.dot(query_head, key_head.T, preferred_element_type=jnp.float32) * (HD ** -0.5)
    query_pos = jnp.arange(SEG)[:, None] + SEG
    key_pos = jnp.arange(2 * SEG)[None, :]
    visible = (key_pos <= query_pos) & (key_pos > query_pos - SEG) & ((key_pos >= SEG) | (first_flag < 1))
    scores = jnp.where(visible, scores, -jnp.inf)
    highest = jnp.max(scores, axis=-1, keepdims=True)
    weights = jnp.exp(scores - highest)
    total = jnp.sum(weights, axis=-1, keepdims=True)
    rounded = weights.astype(jnp.bfloat16)
    summed = jnp.dot(rounded, value_head, preferred_element_type=jnp.float32)
    return summed / total


def segment_attention(packed):
    query_seg, key_seg, value_seg, key_prev, value_prev, first_flag = packed
    key_both = jnp.concatenate([key_prev, key_seg], axis=0)
    value_both = jnp.concatenate([value_prev, value_seg], axis=0)
    flags = jnp.full((HEADS,), first_flag, jnp.int32)
    result = lax.map(window_head, (jnp.transpose(query_seg, (1, 0, 2)), jnp.transpose(key_both, (1, 0, 2)), jnp.transpose(value_both, (1, 0, 2)), flags))
    return jnp.transpose(result, (1, 0, 2))


def segment_terms(packed):
    key_seg, value_seg = packed
    soft_keys = elu_plus(key_seg.astype(jnp.float32)).astype(jnp.bfloat16)
    outer = jnp.einsum("thd,the->hde", soft_keys.astype(jnp.float32), value_seg.astype(jnp.float32))
    totals = jnp.sum(soft_keys.astype(jnp.float32), axis=0)
    return outer, totals


def reference(queries, keys, values, beta, w_out):
    segments = TOKENS // SEG
    shaped = (segments, SEG, HEADS, HD)
    query_all = queries.reshape(shaped)
    key_all = keys.reshape(shaped)
    value_all = values.reshape(shaped)
    terms, norms = lax.map(segment_terms, (key_all, value_all))
    memory = jnp.concatenate([jnp.zeros((1, HEADS, HD, HD), jnp.float32), jnp.cumsum(terms, axis=0)[:-1]], axis=0)
    norm_prev = jnp.concatenate([jnp.zeros((1, HEADS, HD), jnp.float32), jnp.cumsum(norms, axis=0)[:-1]], axis=0)
    soft_queries = lax.optimization_barrier(elu_plus(query_all.astype(jnp.float32)).astype(jnp.bfloat16)).astype(jnp.float32)
    numer = jnp.einsum("sthd,shde->sthe", soft_queries, memory, precision=lax.Precision.HIGHEST)
    denom = 1.0 + jnp.einsum("sthd,shd->sth", soft_queries, norm_prev, precision=lax.Precision.HIGHEST)
    from_memory = numer / denom[..., None]
    zero_seg = jnp.zeros((1, SEG, HEADS, HD), jnp.bfloat16)
    key_prev = jnp.concatenate([zero_seg, key_all[:-1]], axis=0)
    value_prev = jnp.concatenate([zero_seg, value_all[:-1]], axis=0)
    first_flags = (jnp.arange(segments) == 0).astype(jnp.int32)
    local = lax.map(segment_attention, (query_all, key_all, value_all, key_prev, value_prev, first_flags))
    gate = jax.nn.sigmoid(beta.astype(jnp.float32))[None, None, :, None]
    attended = (gate * from_memory + (1.0 - gate) * local).astype(jnp.bfloat16).reshape(TOKENS, HEADS * HD)
    return jnp.dot(attended, w_out, preferred_element_type=jnp.float32).astype(jnp.bfloat16)
```

```python
import functools

import jax
import jax.numpy as jnp
from jax import lax
from jax.experimental import pallas as pl
from jax.experimental.pallas import tpu as pltpu
from jax.sharding import Mesh
from jax.sharding import PartitionSpec as P

HD = 128
ROWS = 256
NB = 8
SEG = NB * ROWS
SEQ = ("seq_0", "seq_1", "seq_2")
MESH = pl.DeviceIdType.MESH
BF = jnp.bfloat16
F32 = jnp.float32
SCALE2 = (HD ** -0.5) * 1.4426950408889634
FIRST = 5


def rows(block):
    return pl.ds(pl.multiple_of(block * ROWS, ROWS), ROWS)


def cols(head):
    return pl.ds(pl.multiple_of(head * HD, HD), HD)


def group_id(block):
    return {"seq_1": block // 2, "seq_2": block % 2}


def phi(x):
    return jnp.where(x > 0, x + 1.0, jnp.exp(jnp.minimum(x, 0.0)))


def body(q_hbm, k_hbm, v_hbm, beta_ref, w_hbm, out_ref,
         kcat, vcat, qh, wv, terms, tmsg, tin, mem, att_out, att_in,
         relay_out, relay_in, part_out, part_in,
         ss, rs, zs, zr, ts, tr, as_, ar, xs, xr, wsem):
    z = lax.axis_index("seq_0")
    y = lax.axis_index("seq_1")
    c = lax.axis_index("seq_2")
    x = lax.axis_index("head")
    nz = lax.axis_size("seq_0")
    place = y * 2 + c
    width = out_ref.shape[1]
    half = width // 2
    znext = lax.rem(z + 1, nz)

    pltpu.make_async_copy(w_hbm, wv, wsem).start()

    barrier = pltpu.get_barrier_semaphore()
    for d in range(1, NB):
        pl.semaphore_signal(barrier, 1, device_id=group_id(lax.rem(place + d, NB)), device_id_type=MESH)
    for d in range(1, 8):
        pl.semaphore_signal(barrier, 1, device_id={"seq_0": lax.rem(z + d, nz)}, device_id_type=MESH)
    for d in (1, 3):
        pl.semaphore_signal(barrier, 1, device_id={"head": lax.rem(x + d, 4)}, device_id_type=MESH)
    pl.semaphore_wait(barrier, NB - 1 + 7 + 2)

    own = SEG + place * ROWS
    targets = (
        (k_hbm, kcat.at[pl.ds(pl.multiple_of(own, ROWS), ROWS), :]),
        (v_hbm, vcat.at[pl.ds(pl.multiple_of(own, ROWS), ROWS), pl.ds(0, HD)]),
        (q_hbm, qh.at[rows(place), :]),
    )

    def to_head(t, chip, core):
        block = chip * 2 + core
        return pltpu.make_async_remote_copy(
            src_ref=targets[t][0].at[:, cols(block)], dst_ref=targets[t][1],
            send_sem=ss.at[t, block], recv_sem=rs.at[t, place],
            device_id={"seq_1": chip, "seq_2": core}, device_id_type=MESH)

    others = [(y, 1 - c)]
    for dy in (1, 3, 2):
        for dc in (0, 1):
            others.append((lax.rem(y + dy, 4), lax.rem(c + dc, 2)))
    for t in (0, 1):
        pltpu.make_async_copy(targets[t][0].at[:, cols(place)], targets[t][1], rs.at[t, place]).start()
    for chip, core in others:
        for t in (0, 1):
            to_head(t, chip, core).start()
    pltpu.make_async_copy(q_hbm.at[:, cols(place)], targets[2][1], rs.at[2, place]).start()
    for chip, core in others:
        to_head(2, chip, core).start()

    vcat[:, HD:] = jnp.ones((2 * SEG, HD), BF)
    terms[...] = jnp.zeros_like(terms)

    code = jnp.where(y == 0, 0 + 3 * 4 + 2 * 16 + 1 * 64,
           jnp.where(y == 1, 1 + 2 * 4 + 3 * 16 + 0 * 64,
           jnp.where(y == 2, 2 + 3 * 4 + 1 * 16 + 0 * 64, 3 + 2 * 4 + 1 * 16 + 0 * 64)))

    def nth(i):
        pair = i // 2
        power = jnp.where(pair == 0, 1, jnp.where(pair == 1, 4, jnp.where(pair == 2, 16, 64)))
        return 2 * lax.rem(code // power, 4) + 1 - lax.rem(i, 2)

    def own_k(p):
        return kcat.at[pl.ds(pl.multiple_of(SEG + p * ROWS, ROWS), ROWS), :]

    def own_v(p):
        return vcat.at[pl.ds(pl.multiple_of(SEG + p * ROWS, ROWS), ROWS), pl.ds(0, HD)]

    def pass_on(t, p):
        src = own_k(p) if t == 0 else own_v(p)
        dst = kcat.at[rows(p), :] if t == 0 else vcat.at[rows(p), pl.ds(0, HD)]
        return pltpu.make_async_remote_copy(
            src_ref=src, dst_ref=dst, send_sem=zs.at[t, p], recv_sem=zr.at[t, p],
            device_id={"seq_0": znext}, device_id_type=MESH)

    def arrived(i):
        p = nth(i)
        pltpu.make_async_copy(own_k(p), own_k(p), rs.at[0, p]).wait()
        pltpu.make_async_copy(own_v(p), own_v(p), rs.at[1, p]).wait()
        return p

    def add_terms(p):
        at = pl.ds(pl.multiple_of(SEG + p * ROWS, ROWS), ROWS)
        soft = phi(kcat[at, :].astype(F32)).astype(BF)
        terms[...] += lax.dot_general(soft, vcat[at, :], (((0,), (0,)), ((), ())), preferred_element_type=F32)

    @pl.loop(0, FIRST)
    def _(i):
        p = arrived(i)
        pass_on(0, p).start()
        pass_on(1, p).start()
        add_terms(p)

    @pl.loop(FIRST, NB)
    def _(i):
        add_terms(arrived(i))

    tmsg[pl.ds(0, HD), :] = terms[:, :HD].astype(BF)
    norm = jnp.transpose(terms[:, HD:])[:8]
    norm_hi = norm.astype(BF)
    norm_lo = (norm - norm_hi.astype(F32)).astype(BF)
    tmsg[pl.ds(HD, 16), :] = jnp.concatenate([norm_hi, norm_lo], axis=0)

    def to_later(other):
        return pltpu.make_async_remote_copy(
            src_ref=tmsg, dst_ref=tin.at[z], send_sem=ts.at[other], recv_sem=tr.at[z],
            device_id={"seq_0": other}, device_id_type=MESH)

    for d in range(1, 8):
        @pl.when(z + d < nz)
        def _():
            to_later(z + d).start()

    @pl.loop(FIRST, NB)
    def _(i):
        p = nth(i)
        pass_on(0, p).start()
        pass_on(1, p).start()

    terms[...] = jnp.zeros_like(terms)

    @pl.loop(0, z)
    def _(other):
        pltpu.make_async_copy(tin.at[other], tin.at[other], tr.at[other]).wait()
        terms[:, :HD] += tin[other, pl.ds(0, HD), :].astype(F32)
        n = tin[other, pl.ds(HD, 16), :].astype(F32)
        terms[pl.ds(0, 8), HD:] += n[:8] + n[8:]

    norm_cols = jnp.transpose(jnp.broadcast_to(terms[0:1, HD:], (HD, HD)))
    full = jnp.concatenate([terms[:, :HD], norm_cols], axis=1)
    full_hi = full.astype(BF)
    mem[pl.ds(0, HD), :] = full_hi
    mem[pl.ds(HD, HD), :] = (full - full_hi.astype(F32)).astype(BF)

    gate = 1.0 / (1.0 + jnp.exp(-jnp.full((8, HD), beta_ref[place], F32)))[0:1]

    def back(j):
        return pltpu.make_async_remote_copy(
            src_ref=att_out.at[j], dst_ref=att_in.at[:, cols(place)],
            send_sem=as_.at[j], recv_sem=ar.at[place],
            device_id=group_id(j), device_id_type=MESH)

    @pl.loop(0, NB)
    def _(jj):
        j = NB - 1 - jj
        pltpu.make_async_copy(kcat.at[rows(j), :], kcat.at[rows(j), :], zr.at[0, j]).wait()
        pltpu.make_async_copy(vcat.at[rows(j), pl.ds(0, HD)], vcat.at[rows(j), pl.ds(0, HD)], zr.at[1, j]).wait()
        pltpu.make_async_copy(qh.at[rows(j), :], qh.at[rows(j), :], rs.at[2, j]).wait()
        q = qh[rows(j), :]
        row = lax.broadcasted_iota(jnp.int32, (ROWS, ROWS), 0)
        col = lax.broadcasted_iota(jnp.int32, (ROWS, ROWS), 1)
        scores, peaks, hidden = [], [], []
        for b in range(NB + 1):
            keys = kcat[pl.ds(pl.multiple_of((j + b) * ROWS, ROWS), ROWS), :]
            s = lax.dot_general(q, keys, (((1,), (1,)), ((), ())), preferred_element_type=F32)
            if b == 0:
                s = jnp.where(col > row, s, -jnp.inf)
            if b == NB:
                s = jnp.where(col <= row, s, -jnp.inf)
            peak = jnp.maximum(s[:, :HD], s[:, HD:])
            gone = (z == 0) & (j + b < NB)
            if b < NB:
                peak = jnp.where(gone, -jnp.inf, peak)
            scores.append(s)
            peaks.append(peak)
            hidden.append(gone)
        top = jnp.max(functools.reduce(jnp.maximum, peaks), axis=1, keepdims=True)
        acc = jnp.zeros((ROWS, 2 * HD), F32)
        for b in range(NB + 1):
            base = top if b == NB else jnp.where(hidden[b], jnp.inf, top)
            weights = jnp.exp2((scores[b] - base) * SCALE2).astype(BF)
            acc += jnp.dot(weights, vcat[pl.ds(pl.multiple_of((j + b) * ROWS, ROWS), ROWS), :],
                           preferred_element_type=F32)
        local = acc[:, :HD] / acc[:, HD:]
        soft = phi(q.astype(F32)).astype(BF)
        past = jnp.dot(jnp.concatenate([soft, soft], axis=1), mem[...], preferred_element_type=F32)
        from_memory = past[:, :HD] / (1.0 + past[:, HD:])
        att_out[j] = (gate * from_memory + (1.0 - gate) * local).astype(BF)

        @pl.when(j != place)
        def _():
            back(j).start()

        @pl.when(j == place)
        def _():
            pltpu.make_async_copy(att_out.at[j], att_in.at[:, cols(place)], ar.at[place]).start()

    @pl.loop(0, NB)
    def _(h):
        pltpu.make_async_copy(att_in.at[:, cols(h)], att_in.at[:, cols(h)], ar.at[h]).wait()

    pltpu.make_async_copy(w_hbm, wv, wsem).wait()

    up, down, far = lax.rem(x + 1, 4), lax.rem(x + 3, 4), lax.rem(x + 2, 4)

    def product(owner, start, size):
        at = pl.ds(pl.multiple_of(owner * width + start, HD), size)
        return jnp.dot(att_in[...], wv[:, at], preferred_element_type=F32)

    def to_x(src, dst, i, target):
        return pltpu.make_async_remote_copy(
            src_ref=src, dst_ref=dst, send_sem=xs.at[i], recv_sem=xr.at[i],
            device_id={"head": target}, device_id_type=MESH)

    copies = []

    def send(src, dst, i, target):
        copy = to_x(src, dst, i, target)
        copy.start()
        copies.append(copy)

    relay_out[0] = product(far, 0, half).astype(BF)
    send(relay_out.at[0], relay_in.at[0], 0, up)
    relay_out[1] = product(far, half, half).astype(BF)
    send(relay_out.at[1], relay_in.at[1], 1, down)
    part_out[1] = product(up, half, half).astype(BF)
    send(part_out.at[1], part_in.at[1], 2, up)
    part_out[2] = product(down, 0, half).astype(BF)
    send(part_out.at[2], part_in.at[2], 3, down)
    first = product(up, 0, half)
    copies[0].wait_recv()
    part_out[0] = (first + relay_in[0].astype(F32)).astype(BF)
    send(part_out.at[0], part_in.at[0], 4, up)
    second = product(down, half, half)
    copies[1].wait_recv()
    part_out[3] = (second + relay_in[1].astype(F32)).astype(BF)
    send(part_out.at[3], part_in.at[3], 5, down)
    left = product(x, 0, half)
    right = product(x, half, half)
    copies[2].wait_recv()
    copies[3].wait_recv()
    left = left + part_in[2].astype(F32)
    right = right + part_in[1].astype(F32)
    copies[4].wait_recv()
    out_ref[:, :half] = (left + part_in[0].astype(F32)).astype(BF)
    copies[5].wait_recv()
    out_ref[:, half:] = (right + part_in[3].astype(F32)).astype(BF)

    for copy in copies:
        copy.wait_send()
    for t in range(3):
        for chip, core in others:
            to_head(t, chip, core).wait_send()

    @pl.loop(0, NB)
    def _(p):
        pass_on(0, p).wait_send()
        pass_on(1, p).wait_send()

        @pl.when(p != place)
        def _():
            back(p).wait_send()

    for d in range(1, 8):
        @pl.when(z + d < nz)
        def _():
            to_later(z + d).wait_send()


def layer(queries, keys, values, beta, w_out):
    tokens, width = queries.shape
    any_space = pl.BlockSpec(memory_space=pl.ANY)
    vmem = pl.BlockSpec(memory_space=pltpu.VMEM)
    dma = pltpu.SemaphoreType.DMA
    half = width // 2
    return pl.pallas_call(
        body,
        name="infini",
        out_shape=jax.ShapeDtypeStruct((tokens, width), BF),
        in_specs=[any_space, any_space, any_space, pl.BlockSpec(memory_space=pltpu.SMEM), any_space],
        out_specs=vmem,
        scratch_shapes=[
            pltpu.VMEM((2 * SEG, HD), BF),
            pltpu.VMEM((2 * SEG, 2 * HD), BF),
            pltpu.VMEM((SEG, HD), BF),
            pltpu.VMEM(w_out.shape, BF),
            pltpu.VMEM((HD, 2 * HD), F32),
            pltpu.VMEM((HD + 16, HD), BF),
            pltpu.VMEM((8, HD + 16, HD), BF),
            pltpu.VMEM((2 * HD, 2 * HD), BF),
            pltpu.VMEM((NB, ROWS, HD), BF),
            pltpu.VMEM((ROWS, NB * HD), BF),
            pltpu.VMEM((2, tokens, half), BF),
            pltpu.VMEM((2, tokens, half), BF),
            pltpu.VMEM((4, tokens, half), BF),
            pltpu.VMEM((4, tokens, half), BF),
            dma((3, NB)), dma((3, NB)),
            dma((2, NB)), dma((2, NB)),
            dma((8,)), dma((8,)),
            dma((NB,)), dma((NB,)),
            dma((6,)), dma((6,)),
            dma(()),
        ],
        compiler_params=pltpu.CompilerParams(
            collective_id=0, has_side_effects=True, vmem_limit_bytes=56 * 1024 * 1024),
    )(queries, keys, values, beta, w_out)


def solution(mesh):
    torus = Mesh(
        mesh.devices.reshape(8, 4, 2, mesh.shape["head"]), ("seq_0", "seq_1", "seq_2", "head")
    )
    return jax.shard_map(
        layer,
        mesh=torus,
        in_specs=(P(SEQ, "head"), P(SEQ, "head"), P(SEQ, "head"), P("head"), P("head", None)),
        out_specs=P(SEQ, "head"),
        check_vma=False,
    )
```

```python
import functools

import jax
import jax.numpy as jnp
from jax import lax
from jax.experimental import pallas as pl
from jax.experimental.pallas import tpu as pltpu
from jax.sharding import Mesh
from jax.sharding import PartitionSpec as P

HD = 128
ROWS = 256
NB = 8
SEG = NB * ROWS
SEQ = ("seq_0", "seq_1", "seq_2")
MESH = pl.DeviceIdType.MESH
BF = jnp.bfloat16
F32 = jnp.float32
SCALE2 = (HD ** -0.5) * 1.4426950408889634
GROUP = 2 * ROWS
GATE_A = 7
GATE_B = 3


def rows(block):
    return pl.ds(pl.multiple_of(block * ROWS, ROWS), ROWS)


def cols(head):
    return pl.ds(pl.multiple_of(head * HD, HD), HD)


def group_id(block):
    return {"seq_1": block // 2, "seq_2": block % 2}


def phi(x):
    return jnp.where(x > 0, x + 1.0, jnp.exp(jnp.minimum(x, 0.0)))


def body(q_hbm, k_hbm, v_hbm, beta_ref, w_hbm, out_ref,
         kcat, vcat, qh, wv, terms, tmsg, tsum, tin, past, mem, top, acc, att_out, att_in,
         relay_out, relay_in, part_out, part_in, staged,
         go, ok, ss, rs, zs, zr, ts, tr, as_, ar, xs, xr, wsem, stage_sem):
    z = lax.axis_index("seq_0")
    y = lax.axis_index("seq_1")
    c = lax.axis_index("seq_2")
    x = lax.axis_index("head")
    place = y * 2 + c
    width = out_ref.shape[1]
    half = width // 2
    quad = lax.rem(z, 4)

    stages = [pltpu.make_async_copy(src, staged.at[i], stage_sem.at[i]) for i, src in enumerate((k_hbm, v_hbm, q_hbm))]
    for copy in stages:
        copy.start()
    pltpu.make_async_copy(w_hbm, wv, wsem).start()

    barrier = pltpu.get_barrier_semaphore()
    is_a, is_b = place == GATE_A, place == GATE_B
    for d in range(1, NB):
        other = lax.rem(place + d, NB)

        @pl.when((other != GATE_A) & (other != GATE_B))
        def _():
            pl.semaphore_signal(barrier, 1, device_id=group_id(other), device_id_type=MESH)

    @pl.when(jnp.logical_not(is_a | is_b))
    def _():
        pl.semaphore_wait(barrier, NB - 1)

    @pl.when((place == GATE_A - 1) | (place == GATE_B - 1))
    def _():
        pl.semaphore_signal(go, 1, device_id=group_id(place + 1), device_id_type=MESH)

    @pl.when(is_a | is_b)
    def _():
        pl.semaphore_wait(go, 1)

    @pl.when(is_a)
    def _():
        @pl.when(z > 0)
        def _():
            pl.semaphore_signal(barrier, 1, device_id={"seq_0": z - 1}, device_id_type=MESH)

        for d in (1, 3):
            pl.semaphore_signal(barrier, 1, device_id={"head": lax.rem(x + d, 4)}, device_id_type=MESH)

    @pl.when(is_b)
    def _():
        for d in (1, 2, 3):
            @pl.when(quad >= d)
            def _():
                pl.semaphore_signal(barrier, 1, device_id={"seq_0": z - d}, device_id_type=MESH)

        @pl.when(z > 3)
        def _():
            pl.semaphore_signal(barrier, 1, device_id={"seq_0": 3}, device_id_type=MESH)

    def pass_word(i, here):
        for d in range(1, NB):
            pl.semaphore_signal(ok.at[i], 1, device_id=group_id(lax.rem(here + d, NB)), device_id_type=MESH)

    own = SEG + place * ROWS
    targets = (
        (staged.at[0], kcat.at[pl.ds(pl.multiple_of(own, ROWS), ROWS), :]),
        (staged.at[1], vcat.at[pl.ds(pl.multiple_of(own, ROWS), ROWS), pl.ds(0, HD)]),
        (staged.at[2], qh.at[rows(place), :]),
    )

    def to_head(t, chip, core):
        block = chip * 2 + core
        return pltpu.make_async_remote_copy(
            src_ref=targets[t][0].at[:, cols(block)], dst_ref=targets[t][1],
            send_sem=ss.at[t, block], recv_sem=rs.at[t, place],
            device_id={"seq_1": chip, "seq_2": core}, device_id_type=MESH)

    others = [(y, 1 - c)]
    for dy in (1, 3, 2):
        for dc in (0, 1):
            others.append((lax.rem(y + dy, 4), lax.rem(c + dc, 2)))
    for t in (0, 1):
        pltpu.make_async_copy((k_hbm, v_hbm)[t].at[:, cols(place)], targets[t][1], rs.at[t, place]).start()
    stages[0].wait()
    stages[1].wait()
    for chip, core in others:
        for t in (0, 1):
            to_head(t, chip, core).start()
    pltpu.make_async_copy(q_hbm.at[:, cols(place)], targets[2][1], rs.at[2, place]).start()
    stages[2].wait()
    for chip, core in others:
        to_head(2, chip, core).start()

    vcat[:, HD:] = jnp.ones((2 * SEG, HD), BF)
    terms[...] = jnp.zeros_like(terms)

    code = jnp.where(y == 0, 0 + 3 * 4 + 2 * 16 + 1 * 64,
           jnp.where(y == 1, 1 + 2 * 4 + 3 * 16 + 0 * 64,
           jnp.where(y == 2, 2 + 3 * 4 + 1 * 16 + 0 * 64, 3 + 2 * 4 + 1 * 16 + 0 * 64)))

    def nth(i):
        pair = i // 2
        power = jnp.where(pair == 0, 1, jnp.where(pair == 1, 4, jnp.where(pair == 2, 16, 64)))
        return 2 * lax.rem(code // power, 4) + 1 - lax.rem(i, 2)

    def own_k(p):
        return kcat.at[pl.ds(pl.multiple_of(SEG + p * ROWS, ROWS), ROWS), :]

    def own_v(p):
        return vcat.at[pl.ds(pl.multiple_of(SEG + p * ROWS, ROWS), ROWS), pl.ds(0, HD)]

    def pass_on(t, p):
        src = own_k(p) if t == 0 else own_v(p)
        dst = kcat.at[rows(p), :] if t == 0 else vcat.at[rows(p), pl.ds(0, HD)]
        return pltpu.make_async_remote_copy(
            src_ref=src, dst_ref=dst, send_sem=zs.at[t, p], recv_sem=zr.at[t, p],
            device_id={"seq_0": z + 1}, device_id_type=MESH)

    def arrived(i):
        p = nth(i)
        pltpu.make_async_copy(own_k(p), own_k(p), rs.at[0, p]).wait()
        pltpu.make_async_copy(own_v(p), own_v(p), rs.at[1, p]).wait()
        return p

    def add_terms(p):
        at = pl.ds(pl.multiple_of(SEG + p * ROWS, ROWS), ROWS)
        soft = phi(kcat[at, :].astype(F32)).astype(BF)
        terms[...] += lax.dot_general(soft, vcat[at, :], (((0,), (0,)), ((), ())), preferred_element_type=F32)

    @pl.when(is_a)
    def _():
        pl.semaphore_wait(barrier, jnp.where(z < 7, 3, 2))
        pass_word(0, GATE_A)

    @pl.when(jnp.logical_not(is_a))
    def _():
        pl.semaphore_wait(ok.at[0], 1)

    def forward(p):
        @pl.when(z < 7)
        def _():
            pass_on(0, p).start()
            pass_on(1, p).start()

    @pl.loop(0, 4)
    def _(i):
        p = arrived(i)
        forward(p)
        add_terms(p)

    @pl.loop(4, NB)
    def _(i):
        add_terms(arrived(i))

    hears = 3 - quad + jnp.where(z == 3, 4, 0)

    @pl.when(is_b)
    def _():
        @pl.when(hears > 0)
        def _():
            pl.semaphore_wait(barrier, hears)

        pass_word(1, GATE_B)

    @pl.when(jnp.logical_not(is_b))
    def _():
        pl.semaphore_wait(ok.at[1], 1)

    def put(dst, block, norm):
        dst[pl.ds(0, HD), :] = block.astype(BF)
        norm_hi = norm.astype(BF)
        norm_lo = (norm - norm_hi.astype(F32)).astype(BF)
        dst[pl.ds(HD, 16), :] = jnp.concatenate([norm_hi, norm_lo], axis=0)

    def add_in(slot):
        pltpu.make_async_copy(tin.at[slot], tin.at[slot], tr.at[slot]).wait()
        past[:, :HD] += tin[slot, pl.ds(0, HD), :].astype(F32)
        n = tin[slot, pl.ds(HD, 16), :].astype(F32)
        past[pl.ds(0, 8), HD:] += n[:8] + n[8:]

    def to_quad(d):
        return pltpu.make_async_remote_copy(
            src_ref=tmsg, dst_ref=tin.at[quad], send_sem=ts.at[d], recv_sem=tr.at[quad],
            device_id={"seq_0": z + d}, device_id_type=MESH)

    def to_upper(d):
        return pltpu.make_async_remote_copy(
            src_ref=tsum, dst_ref=tin.at[4], send_sem=ts.at[3 + d], recv_sem=tr.at[4],
            device_id={"seq_0": z + d}, device_id_type=MESH)

    norm_rows = jnp.transpose(terms[:, HD:])[:8]
    put(tmsg, terms[:, :HD], norm_rows)
    past[...] = jnp.zeros_like(past)
    for d in (1, 2, 3):
        @pl.when(quad + d < 4)
        def _():
            to_quad(d).start()

    @pl.loop(4, 6)
    def _(i):
        forward(nth(i))

    @pl.when(z == 3)
    def _():
        for slot in range(3):
            add_in(slot)
        put(tsum, past[:, :HD] + terms[:, :HD], past[pl.ds(0, 8), HD:] + jnp.transpose(terms[:, HD:])[:8])
        for d in (1, 2, 3, 4):
            to_upper(d).start()

    @pl.loop(6, NB)
    def _(i):
        forward(nth(i))

    gate = 1.0 / (1.0 + jnp.exp(-jnp.full((8, HD), beta_ref[place], F32)))[0:1]

    def back(j):
        return pltpu.make_async_remote_copy(
            src_ref=att_out.at[rows(j), :], dst_ref=att_in.at[:, cols(place)],
            send_sem=as_.at[j], recv_sem=ar.at[place],
            device_id=group_id(j), device_id_type=MESH)

    row = lax.broadcasted_iota(jnp.int32, (ROWS, ROWS), 0)
    col = lax.broadcasted_iota(jnp.int32, (ROWS, ROWS), 1)

    def at_rows(start):
        return pl.ds(pl.multiple_of(start, ROWS), ROWS)

    def meet(*jobs):
        held = [None] * len(jobs)

        def score(n):
            j, blocks, first = jobs[n]
            q = qh[rows(j), :]
            old = None if first else top[rows(j), :]
            scores = []
            for start, mask in blocks:
                s = lax.dot_general(q, kcat[at_rows(start), :], (((1,), (1,)), ((), ())), preferred_element_type=F32)
                if mask == "le":
                    s = jnp.where(col <= row, s, -jnp.inf)
                elif mask == "gt":
                    s = jnp.where(col > row, s, -jnp.inf)
                scores.append(s)
            held[n] = (old, scores)

        def soften(n):
            old, scores = held[n]
            peak = functools.reduce(jnp.maximum, [s[:, i * HD:(i + 1) * HD] for s in scores for i in (0, 1)])
            peak = jnp.broadcast_to(jnp.max(peak, axis=1, keepdims=True), (ROWS, HD))
            fade = None
            if old is not None:
                peak = jnp.maximum(old, peak)
                fade = jnp.exp2((old - peak) * SCALE2)
            both = jnp.concatenate([peak, peak], axis=1)
            held[n] = (peak, fade, [jnp.exp2((s - both) * SCALE2).astype(BF) for s in scores])

        def gather(n):
            j, blocks, _ = jobs[n]
            peak, fade, weights = held[n]
            out = None
            for w, (start, _) in zip(weights, blocks):
                more = jnp.dot(w, vcat[at_rows(start), :], preferred_element_type=F32)
                out = more if out is None else out + more
            if fade is not None:
                out = acc[rows(j), :] * jnp.concatenate([fade, fade], axis=1) + out
            acc[rows(j), :] = out
            held[n] = peak

        for n in range(len(jobs) + 2):
            if n < len(jobs):
                score(n)
            if 0 <= n - 1 < len(jobs):
                soften(n - 1)
            if n >= 2:
                gather(n - 2)
        for (j, _, _), peak in zip(jobs, held):
            top[rows(j), :] = peak

    def own_diagonal(g):
        base = SEG + g * GROUP
        return [(2 * g, [(base, "le")], True), (2 * g + 1, [(base, None), (base + ROWS, "le")], True)]

    def whole(g, base):
        return [(2 * g + i, [(base, None), (base + ROWS, None)], False) for i in (0, 1)]

    def previous_diagonal(g):
        base = g * GROUP
        return [(2 * g, [(base, "gt"), (base + ROWS, None)], False), (2 * g + 1, [(base + ROWS, "gt")], False)]

    @pl.loop(0, 2)
    def _(i):
        for k in range(4):
            j = 4 * i + k
            pltpu.make_async_copy(qh.at[rows(j), :], qh.at[rows(j), :], rs.at[2, j]).wait()
        meet(*own_diagonal(2 * i), *own_diagonal(2 * i + 1))

    @pl.loop(0, 3)
    def _(i):
        meet(*whole(3, SEG + i * GROUP), *whole(jnp.minimum(1 + i, 2), SEG + jnp.maximum(i - 1, 0) * GROUP))

    @pl.when(z != 3)
    def _():
        @pl.loop(0, quad)
        def _(slot):
            add_in(slot)

        @pl.when(z > 3)
        def _():
            add_in(4)

    norm_cols = jnp.transpose(jnp.broadcast_to(past[0:1, HD:], (HD, HD)))
    full = jnp.concatenate([past[:, :HD], norm_cols], axis=1)
    full_hi = full.astype(BF)
    mem[pl.ds(0, HD), :] = full_hi
    mem[pl.ds(HD, HD), :] = (full - full_hi.astype(F32)).astype(BF)

    def finish(j):
        local = acc[rows(j), :HD] / acc[rows(j), HD:]
        soft = phi(qh[rows(j), :].astype(F32)).astype(BF)
        found = jnp.dot(jnp.concatenate([soft, soft], axis=1), mem[...], preferred_element_type=F32)
        from_memory = found[:, :HD] / (1.0 + found[:, HD:])
        att_out[rows(j), :] = (gate * from_memory + (1.0 - gate) * local).astype(BF)

        @pl.when(j != place)
        def _():
            back(j).start()

        @pl.when(j == place)
        def _():
            pltpu.make_async_copy(att_out.at[rows(j), :], att_in.at[:, cols(place)], ar.at[place]).start()

    complete = jnp.where(y == 0, 3 + 3 * 4 + 2 * 16 + 1 * 64,
               jnp.where(y == 1, 3 + 2 * 4 + 2 * 16 + 2 * 64,
               jnp.where(y == 2, 3 + 2 * 4 + 1 * 16 + 1 * 64, 3 + 2 * 4 + 1 * 16 + 0 * 64)))

    @pl.loop(0, 4)
    def _(i):
        g = nth(2 * i) // 2

        @pl.when(z > 0)
        def _():
            for j in (2 * g, 2 * g + 1):
                pltpu.make_async_copy(kcat.at[rows(j), :], kcat.at[rows(j), :], zr.at[0, j]).wait()
                pltpu.make_async_copy(vcat.at[rows(j), pl.ds(0, HD)], vcat.at[rows(j), pl.ds(0, HD)], zr.at[1, j]).wait()

            @pl.when(g == 0)
            def _():
                meet(*previous_diagonal(0))

            @pl.when(g > 0)
            def _():
                meet(*previous_diagonal(g), *whole(0, g * GROUP))

            @pl.when(g == 2)
            def _():
                meet(*whole(1, 2 * GROUP))

            @pl.when(g == 3)
            def _():
                meet(*whole(1, 3 * GROUP), *whole(2, 3 * GROUP))

        @pl.loop(0, NB)
        def _(jj):
            j = NB - 1 - jj
            pair = j // 2
            power = jnp.where(pair == 0, 1, jnp.where(pair == 1, 4, jnp.where(pair == 2, 16, 64)))

            @pl.when(lax.rem(complete // power, 4) == i)
            def _():
                finish(j)

    @pl.loop(0, NB)
    def _(h):
        pltpu.make_async_copy(att_in.at[:, cols(h)], att_in.at[:, cols(h)], ar.at[h]).wait()

    pltpu.make_async_copy(w_hbm, wv, wsem).wait()

    up, down, far = lax.rem(x + 1, 4), lax.rem(x + 3, 4), lax.rem(x + 2, 4)

    def product(owner, start, size):
        at = pl.ds(pl.multiple_of(owner * width + start, HD), size)
        return jnp.dot(att_in[...], wv[:, at], preferred_element_type=F32)

    def to_x(src, dst, i, target):
        return pltpu.make_async_remote_copy(
            src_ref=src, dst_ref=dst, send_sem=xs.at[i], recv_sem=xr.at[i],
            device_id={"head": target}, device_id_type=MESH)

    copies = []

    def send(src, dst, i, target):
        copy = to_x(src, dst, i, target)
        copy.start()
        copies.append(copy)

    relay_out[0] = product(far, 0, half).astype(BF)
    send(relay_out.at[0], relay_in.at[0], 0, up)
    relay_out[1] = product(far, half, half).astype(BF)
    send(relay_out.at[1], relay_in.at[1], 1, down)
    part_out[1] = product(up, half, half).astype(BF)
    send(part_out.at[1], part_in.at[1], 2, up)
    part_out[2] = product(down, 0, half).astype(BF)
    send(part_out.at[2], part_in.at[2], 3, down)
    first = product(up, 0, half)
    copies[0].wait_recv()
    part_out[0] = (first + relay_in[0].astype(F32)).astype(BF)
    send(part_out.at[0], part_in.at[0], 4, up)
    second = product(down, half, half)
    copies[1].wait_recv()
    part_out[3] = (second + relay_in[1].astype(F32)).astype(BF)
    send(part_out.at[3], part_in.at[3], 5, down)
    left = product(x, 0, half)
    right = product(x, half, half)
    copies[2].wait_recv()
    copies[3].wait_recv()
    left = left + part_in[2].astype(F32)
    right = right + part_in[1].astype(F32)
    copies[4].wait_recv()
    out_ref[:, :half] = (left + part_in[0].astype(F32)).astype(BF)
    copies[5].wait_recv()
    out_ref[:, half:] = (right + part_in[3].astype(F32)).astype(BF)

    for copy in copies:
        copy.wait_send()
    for t in range(3):
        for chip, core in others:
            to_head(t, chip, core).wait_send()

    @pl.loop(0, NB)
    def _(p):
        @pl.when(z < 7)
        def _():
            pass_on(0, p).wait_send()
            pass_on(1, p).wait_send()

        @pl.when(p != place)
        def _():
            back(p).wait_send()

    for d in (1, 2, 3):
        @pl.when(quad + d < 4)
        def _():
            to_quad(d).wait_send()

    @pl.when(z == 3)
    def _():
        for d in (1, 2, 3, 4):
            to_upper(d).wait_send()


def layer(queries, keys, values, beta, w_out):
    tokens, width = queries.shape
    any_space = pl.BlockSpec(memory_space=pl.ANY)
    vmem = pl.BlockSpec(memory_space=pltpu.VMEM)
    dma = pltpu.SemaphoreType.DMA
    half = width // 2
    return pl.pallas_call(
        body,
        name="infini",
        out_shape=jax.ShapeDtypeStruct((tokens, width), BF),
        in_specs=[any_space, any_space, any_space, pl.BlockSpec(memory_space=pltpu.SMEM), any_space],
        out_specs=vmem,
        scratch_shapes=[
            pltpu.VMEM((2 * SEG, HD), BF),
            pltpu.VMEM((2 * SEG, 2 * HD), BF),
            pltpu.VMEM((SEG, HD), BF),
            pltpu.VMEM(w_out.shape, BF),
            pltpu.VMEM((HD, 2 * HD), F32),
            pltpu.VMEM((HD + 16, HD), BF),
            pltpu.VMEM((HD + 16, HD), BF),
            pltpu.VMEM((5, HD + 16, HD), BF),
            pltpu.VMEM((HD, 2 * HD), F32),
            pltpu.VMEM((2 * HD, 2 * HD), BF),
            pltpu.VMEM((SEG, HD), F32),
            pltpu.VMEM((SEG, 2 * HD), F32),
            pltpu.VMEM((SEG, HD), BF),
            pltpu.VMEM((ROWS, NB * HD), BF),
            pltpu.VMEM((2, tokens, half), BF),
            pltpu.VMEM((2, tokens, half), BF),
            pltpu.VMEM((4, tokens, half), BF),
            pltpu.VMEM((4, tokens, half), BF),
            pltpu.VMEM((3, tokens, width), BF),
            pltpu.SemaphoreType.REGULAR, pltpu.SemaphoreType.REGULAR((2,)),
            dma((3, NB)), dma((3, NB)),
            dma((2, NB)), dma((2, NB)),
            dma((8,)), dma((8,)),
            dma((NB,)), dma((NB,)),
            dma((6,)), dma((6,)),
            dma(()), dma((3,)),
        ],
        compiler_params=pltpu.CompilerParams(
            collective_id=0, has_side_effects=True, vmem_limit_bytes=56 * 1024 * 1024),
    )(queries, keys, values, beta, w_out)


def solution(mesh):
    torus = Mesh(
        mesh.devices.reshape(8, 4, 2, mesh.shape["head"]), ("seq_0", "seq_1", "seq_2", "head")
    )
    return jax.shard_map(
        layer,
        mesh=torus,
        in_specs=(P(SEQ, "head"), P(SEQ, "head"), P(SEQ, "head"), P("head"), P("head", None)),
        out_specs=P(SEQ, "head"),
        check_vma=False,
    )
```

```python
import functools

import jax
import jax.numpy as jnp
from jax import lax
from jax.experimental import pallas as pl
from jax.experimental.pallas import tpu as pltpu
from jax.sharding import Mesh
from jax.sharding import PartitionSpec as P

HD = 128
ROWS = 256
NB = 8
SEG = NB * ROWS
SEQ = ("seq_0", "seq_1", "seq_2")
MESH = pl.DeviceIdType.MESH
BF = jnp.bfloat16
F32 = jnp.float32
SCALE2 = (HD ** -0.5) * 1.4426950408889634
GROUP = 2 * ROWS


def aligned(start, size):
    return start if isinstance(start, int) else pl.multiple_of(start, size)


def rows(block):
    return pl.ds(aligned(block * ROWS, ROWS), ROWS)


def cols(head):
    return pl.ds(aligned(head * HD, HD), HD)


def group_id(block):
    return {"seq_1": block // 2, "seq_2": block % 2}


def phi(x):
    return jnp.where(x > 0, x + 1.0, jnp.exp(jnp.minimum(x, 0.0)))


def body(q_hbm, k_hbm, v_hbm, beta_ref, w_hbm, out_ref,
         kcat, vcat, qh, wv, terms, tmsg, tsum, tin, past, mem, top, acc, att_out, att_in,
         relay_out, relay_in, part_out, part_in, staged,
         go, ok, up, ss, rs, zs, zr, ts, tr, as_, ar, xs, xr, wsem, stage_sem):
    z = lax.axis_index("seq_0")
    y = lax.axis_index("seq_1")
    c = lax.axis_index("seq_2")
    x = lax.axis_index("head")
    place = y * 2 + c
    width = out_ref.shape[1]
    half = width // 2
    quad = lax.rem(z, 4)

    stages = [pltpu.make_async_copy(src, staged.at[i], stage_sem.at[i]) for i, src in enumerate((k_hbm, v_hbm, q_hbm))]
    for copy in stages:
        copy.start()
    pltpu.make_async_copy(w_hbm, wv, wsem).start()

    barrier = pltpu.get_barrier_semaphore()
    for d in range(1, NB):
        other = lax.rem(place + d, NB)

        @pl.when(lax.rem(other, 2) == 0)
        def _():
            pl.semaphore_signal(barrier, 1, device_id=group_id(other), device_id_type=MESH)

    @pl.when(c == 0)
    def _():
        pl.semaphore_wait(barrier, NB - 1)
        pl.semaphore_signal(go, 1, device_id={"seq_2": 1}, device_id_type=MESH)

    @pl.when(c == 1)
    def _():
        pl.semaphore_wait(go, 1)

        @pl.when(z > 0)
        def _():
            pl.semaphore_signal(barrier, 1, device_id={"seq_0": z - 1}, device_id_type=MESH)

        @pl.when(z < 7)
        def _():
            pl.semaphore_signal(barrier, 1, device_id={"seq_0": z + 1}, device_id_type=MESH)

        for d in (1, 3):
            pl.semaphore_signal(barrier, 1, device_id={"head": lax.rem(x + d, 4)}, device_id_type=MESH)

    def pass_word(i):
        pl.semaphore_signal(ok.at[i], 1, device_id={"seq_2": 0}, device_id_type=MESH)

    def hear_of(i):
        @pl.when((c == 1) & (z <= 5 - i))
        def _():
            pl.semaphore_wait(up.at[i], 1)

            if i < 2:
                @pl.when(z > 0)
                def _():
                    pl.semaphore_signal(up.at[i + 1], 1, device_id={"seq_0": z - 1}, device_id_type=MESH)

    own = SEG + place * ROWS
    targets = (
        (staged.at[0], kcat.at[pl.ds(pl.multiple_of(own, ROWS), ROWS), :]),
        (staged.at[1], vcat.at[pl.ds(pl.multiple_of(own, ROWS), ROWS), pl.ds(0, HD)]),
        (staged.at[2], qh.at[rows(place), :]),
    )

    def to_head(t, chip, core):
        block = chip * 2 + core
        return pltpu.make_async_remote_copy(
            src_ref=targets[t][0].at[:, cols(block)], dst_ref=targets[t][1],
            send_sem=ss.at[t, block], recv_sem=rs.at[t, place],
            device_id={"seq_1": chip, "seq_2": core}, device_id_type=MESH)

    others = [(y, 1 - c)]
    for dy in (1, 3, 2):
        for dc in (0, 1):
            others.append((lax.rem(y + dy, 4), lax.rem(c + dc, 2)))
    for t in (0, 1):
        pltpu.make_async_copy((k_hbm, v_hbm)[t].at[:, cols(place)], targets[t][1], rs.at[t, place]).start()
    stages[0].wait()
    stages[1].wait()
    for chip, core in others[:5]:
        for t in (0, 1):
            to_head(t, chip, core).start()
    pltpu.make_async_copy(q_hbm.at[:, cols(place)], targets[2][1], rs.at[2, place]).start()
    stages[2].wait()
    to_head(2, y, 1 - c).start()

    @pl.when(c == 1)
    def _():
        pl.semaphore_wait(barrier, 2 + jnp.where(z < 7, 1, 0) + jnp.where(z > 0, 1, 0))
        pass_word(0)

        @pl.when((z > 0) & (z < 7))
        def _():
            pl.semaphore_signal(up.at[0], 1, device_id={"seq_0": z - 1}, device_id_type=MESH)

    @pl.when(c == 0)
    def _():
        pl.semaphore_wait(ok.at[0], 1)

    vcat[:, HD:] = jnp.ones((2 * SEG, HD), BF)
    terms[...] = jnp.zeros_like(terms)

    code = jnp.where(y == 0, 0 + 3 * 4 + 2 * 16 + 1 * 64,
           jnp.where(y == 1, 1 + 2 * 4 + 3 * 16 + 0 * 64,
           jnp.where(y == 2, 2 + 3 * 4 + 1 * 16 + 0 * 64, 3 + 2 * 4 + 1 * 16 + 0 * 64)))

    def nth(i):
        pair = i // 2
        power = jnp.where(pair == 0, 1, jnp.where(pair == 1, 4, jnp.where(pair == 2, 16, 64)))
        return 2 * lax.rem(code // power, 4) + 1 - lax.rem(i, 2)

    def own_k(p):
        return kcat.at[pl.ds(pl.multiple_of(SEG + p * ROWS, ROWS), ROWS), :]

    def own_v(p):
        return vcat.at[pl.ds(pl.multiple_of(SEG + p * ROWS, ROWS), ROWS), pl.ds(0, HD)]

    def pass_on(t, p):
        src = own_k(p) if t == 0 else own_v(p)
        dst = kcat.at[rows(p), :] if t == 0 else vcat.at[rows(p), pl.ds(0, HD)]
        return pltpu.make_async_remote_copy(
            src_ref=src, dst_ref=dst, send_sem=zs.at[t, p], recv_sem=zr.at[t, p],
            device_id={"seq_0": z + 1}, device_id_type=MESH)

    def arrived(i):
        p = nth(i)
        pltpu.make_async_copy(own_k(p), own_k(p), rs.at[0, p]).wait()
        pltpu.make_async_copy(own_v(p), own_v(p), rs.at[1, p]).wait()
        return p

    def add_terms(p):
        at = pl.ds(pl.multiple_of(SEG + p * ROWS, ROWS), ROWS)
        soft = phi(kcat[at, :].astype(F32)).astype(BF)
        terms[...] += lax.dot_general(soft, vcat[at, :], (((0,), (0,)), ((), ())), preferred_element_type=F32)

    def forward(p):
        @pl.when(z < 7)
        def _():
            pass_on(0, p).start()
            pass_on(1, p).start()

    @pl.loop(0, 2)
    def _(i):
        p = arrived(i)
        forward(p)
        add_terms(p)

    for chip, core in others[5:]:
        for t in (0, 1):
            to_head(t, chip, core).start()
    hear_of(0)

    @pl.loop(2, 4)
    def _(i):
        p = arrived(i)
        forward(p)
        add_terms(p)

    for chip, core in others[1:]:
        to_head(2, chip, core).start()
    hear_of(1)

    @pl.loop(4, NB)
    def _(i):
        add_terms(arrived(i))

    hear_of(2)

    @pl.when(c == 1)
    def _():
        pass_word(1)

    @pl.when(c == 0)
    def _():
        pl.semaphore_wait(ok.at[1], 1)

    def put(dst, block, norm):
        dst[pl.ds(0, HD), :] = block.astype(BF)
        norm_hi = norm.astype(BF)
        norm_lo = (norm - norm_hi.astype(F32)).astype(BF)
        dst[pl.ds(HD, 16), :] = jnp.concatenate([norm_hi, norm_lo], axis=0)

    def add_in(slot):
        pltpu.make_async_copy(tin.at[slot], tin.at[slot], tr.at[slot]).wait()
        past[:, :HD] += tin[slot, pl.ds(0, HD), :].astype(F32)
        n = tin[slot, pl.ds(HD, 16), :].astype(F32)
        past[pl.ds(0, 8), HD:] += n[:8] + n[8:]

    def to_quad(d):
        return pltpu.make_async_remote_copy(
            src_ref=tmsg, dst_ref=tin.at[quad], send_sem=ts.at[d], recv_sem=tr.at[quad],
            device_id={"seq_0": z + d}, device_id_type=MESH)

    def to_upper(d):
        return pltpu.make_async_remote_copy(
            src_ref=tsum, dst_ref=tin.at[4], send_sem=ts.at[3 + d], recv_sem=tr.at[4],
            device_id={"seq_0": z + d}, device_id_type=MESH)

    norm_rows = jnp.transpose(terms[:, HD:])[:8]
    put(tmsg, terms[:, :HD], norm_rows)
    past[...] = jnp.zeros_like(past)
    for d in (1, 2, 3):
        @pl.when(quad + d < 4)
        def _():
            to_quad(d).start()

    @pl.loop(4, 6)
    def _(i):
        forward(nth(i))

    gate = 1.0 / (1.0 + jnp.exp(-jnp.full((8, HD), beta_ref[place], F32)))[0:1]

    def back(j):
        return pltpu.make_async_remote_copy(
            src_ref=att_out.at[rows(j), :], dst_ref=att_in.at[:, cols(place)],
            send_sem=as_.at[j], recv_sem=ar.at[place],
            device_id=group_id(j), device_id_type=MESH)

    row = lax.broadcasted_iota(jnp.int32, (ROWS, ROWS), 0)
    col = lax.broadcasted_iota(jnp.int32, (ROWS, ROWS), 1)

    def at_rows(start):
        return pl.ds(aligned(start, ROWS), ROWS)

    def meet(*jobs):
        held = [None] * len(jobs)

        def score(n):
            j, blocks, first = jobs[n]
            q = qh[rows(j), :]
            old = None if first else top[rows(j), :]
            scores = []
            for start, mask in blocks:
                s = lax.dot_general(q, kcat[at_rows(start), :], (((1,), (1,)), ((), ())), preferred_element_type=F32)
                if mask == "le":
                    s = jnp.where(col <= row, s, -jnp.inf)
                elif mask == "gt":
                    s = jnp.where(col > row, s, -jnp.inf)
                scores.append(s)
            held[n] = (old, scores)

        def soften(n):
            old, scores = held[n]
            peak = functools.reduce(jnp.maximum, [s[:, i * HD:(i + 1) * HD] for s in scores for i in (0, 1)])
            peak = jnp.broadcast_to(jnp.max(peak, axis=1, keepdims=True), (ROWS, HD))
            fade = None
            if old is not None:
                peak = jnp.maximum(old, peak)
                fade = jnp.exp2((old - peak) * SCALE2)
            both = jnp.concatenate([peak, peak], axis=1)
            held[n] = (peak, fade, [jnp.exp2((s - both) * SCALE2).astype(BF) for s in scores])

        def gather(n):
            j, blocks, _ = jobs[n]
            peak, fade, weights = held[n]
            out = None
            for w, (start, _) in zip(weights, blocks):
                more = jnp.dot(w, vcat[at_rows(start), :], preferred_element_type=F32)
                out = more if out is None else out + more
            if fade is not None:
                out = acc[rows(j), :] * jnp.concatenate([fade, fade], axis=1) + out
            acc[rows(j), :] = out
            held[n] = peak

        for n in range(len(jobs) + 2):
            if n < len(jobs):
                score(n)
            if 0 <= n - 1 < len(jobs):
                soften(n - 1)
            if n >= 2:
                gather(n - 2)
        for (j, _, _), peak in zip(jobs, held):
            top[rows(j), :] = peak

    def whole(g, base):
        return [(2 * g + i, [(base, None), (base + ROWS, None)], False) for i in (0, 1)]

    def previous_diagonal(g):
        base = g * GROUP
        return [(2 * g, [(base, "gt"), (base + ROWS, None)], False), (2 * g + 1, [(base + ROWS, "gt")], False)]

    near = jnp.where(y == 0, 0 + 3 * 4 + 1 * 16 + 2 * 64,
           jnp.where(y == 1, 1 + 2 * 4 + 0 * 16 + 3 * 64,
           jnp.where(y == 2, 2 + 3 * 4 + 1 * 16 + 0 * 64, 3 + 2 * 4 + 0 * 16 + 1 * 64)))

    @pl.loop(0, 4)
    def _(i):
        power = jnp.where(i == 0, 1, jnp.where(i == 1, 4, jnp.where(i == 2, 16, 64)))
        g = lax.rem(near // power, 4)
        for j in (2 * g, 2 * g + 1):
            pltpu.make_async_copy(qh.at[rows(j), :], qh.at[rows(j), :], rs.at[2, j]).wait()
        for own_g in range(4):
            @pl.when(g == own_g)
            def _():
                meet(*[(j, [(SEG + k * ROWS, None) for k in range(j)] + [(SEG + j * ROWS, "le")], True)
                       for j in (2 * own_g, 2 * own_g + 1)])

        @pl.when(i == 1)
        def _():
            @pl.when(z == 3)
            def _():
                for slot in range(3):
                    add_in(slot)
                put(tsum, past[:, :HD] + terms[:, :HD], past[pl.ds(0, 8), HD:] + jnp.transpose(terms[:, HD:])[:8])
                for d in (1, 2, 3, 4):
                    to_upper(d).start()

            for k in (6, 7):
                forward(nth(k))

    def finish(j):
        local = acc[rows(j), :HD] / acc[rows(j), HD:]
        soft = phi(qh[rows(j), :].astype(F32)).astype(BF)
        found = jnp.dot(jnp.concatenate([soft, soft], axis=1), mem[...], preferred_element_type=F32)
        from_memory = found[:, :HD] / (1.0 + found[:, HD:])
        att_out[rows(j), :] = (gate * from_memory + (1.0 - gate) * local).astype(BF)

        @pl.when(j != place)
        def _():
            back(j).start()

        @pl.when(j == place)
        def _():
            pltpu.make_async_copy(att_out.at[rows(j), :], att_in.at[:, cols(place)], ar.at[place]).start()

    def came(j):
        pltpu.make_async_copy(kcat.at[rows(j), :], kcat.at[rows(j), :], zr.at[0, j]).wait()
        pltpu.make_async_copy(vcat.at[rows(j), pl.ds(0, HD)], vcat.at[rows(j), pl.ds(0, HD)], zr.at[1, j]).wait()

    def meet_previous(g):
        @pl.when(z > 0)
        def _():
            came(2 * g + 1)
            came(2 * g)
            jobs = previous_diagonal(g)
            for k in range(g):
                jobs = jobs + whole(k, g * GROUP)
            meet(*jobs)

    meet_previous(3)
    meet_previous(2)

    @pl.when(z != 3)
    def _():
        @pl.loop(0, quad)
        def _(slot):
            add_in(slot)

        @pl.when(z > 3)
        def _():
            add_in(4)

    norm_cols = jnp.transpose(jnp.broadcast_to(past[0:1, HD:], (HD, HD)))
    full = jnp.concatenate([past[:, :HD], norm_cols], axis=1)
    full_hi = full.astype(BF)
    mem[pl.ds(0, HD), :] = full_hi
    mem[pl.ds(HD, HD), :] = (full - full_hi.astype(F32)).astype(BF)

    @pl.loop(0, 4)
    def _(i):
        finish(7 - i)

    @pl.when(y == 0)
    def _():
        meet_previous(0)
        meet_previous(1)

        @pl.loop(0, 4)
        def _(j):
            finish(j)

    @pl.when(y != 0)
    def _():
        meet_previous(1)

        @pl.loop(2, 4)
        def _(j):
            finish(j)

        @pl.when(z > 0)
        def _():
            came(1)
            meet((1, [(ROWS, "gt")], False), (0, [(ROWS, None)], False))

        finish(1)

        @pl.when(z > 0)
        def _():
            came(0)
            meet((0, [(0, "gt")], False))

        finish(0)

    @pl.loop(0, NB)
    def _(h):
        pltpu.make_async_copy(att_in.at[:, cols(h)], att_in.at[:, cols(h)], ar.at[h]).wait()

    pltpu.make_async_copy(w_hbm, wv, wsem).wait()

    up, down, far = lax.rem(x + 1, 4), lax.rem(x + 3, 4), lax.rem(x + 2, 4)

    def product(owner, start, size):
        at = pl.ds(pl.multiple_of(owner * width + start, HD), size)
        return jnp.dot(att_in[...], wv[:, at], preferred_element_type=F32)

    def to_x(src, dst, i, target):
        return pltpu.make_async_remote_copy(
            src_ref=src, dst_ref=dst, send_sem=xs.at[i], recv_sem=xr.at[i],
            device_id={"head": target}, device_id_type=MESH)

    copies = []

    def send(src, dst, i, target):
        copy = to_x(src, dst, i, target)
        copy.start()
        copies.append(copy)

    relay_out[0] = product(far, 0, half).astype(BF)
    send(relay_out.at[0], relay_in.at[0], 0, up)
    relay_out[1] = product(far, half, half).astype(BF)
    send(relay_out.at[1], relay_in.at[1], 1, down)
    part_out[1] = product(up, half, half).astype(BF)
    send(part_out.at[1], part_in.at[1], 2, up)
    part_out[2] = product(down, 0, half).astype(BF)
    send(part_out.at[2], part_in.at[2], 3, down)
    first = product(up, 0, half)
    copies[0].wait_recv()
    part_out[0] = (first + relay_in[0].astype(F32)).astype(BF)
    send(part_out.at[0], part_in.at[0], 4, up)
    second = product(down, half, half)
    copies[1].wait_recv()
    part_out[3] = (second + relay_in[1].astype(F32)).astype(BF)
    send(part_out.at[3], part_in.at[3], 5, down)
    left = product(x, 0, half)
    right = product(x, half, half)
    copies[2].wait_recv()
    copies[3].wait_recv()
    left = left + part_in[2].astype(F32)
    right = right + part_in[1].astype(F32)
    copies[4].wait_recv()
    out_ref[:, :half] = (left + part_in[0].astype(F32)).astype(BF)
    copies[5].wait_recv()
    out_ref[:, half:] = (right + part_in[3].astype(F32)).astype(BF)

    for copy in copies:
        copy.wait_send()
    for t in range(3):
        for chip, core in others:
            to_head(t, chip, core).wait_send()

    @pl.loop(0, NB)
    def _(p):
        @pl.when(z < 7)
        def _():
            pass_on(0, p).wait_send()
            pass_on(1, p).wait_send()

        @pl.when(p != place)
        def _():
            back(p).wait_send()

    for d in (1, 2, 3):
        @pl.when(quad + d < 4)
        def _():
            to_quad(d).wait_send()

    @pl.when(z == 3)
    def _():
        for d in (1, 2, 3, 4):
            to_upper(d).wait_send()


def layer(queries, keys, values, beta, w_out):
    tokens, width = queries.shape
    any_space = pl.BlockSpec(memory_space=pl.ANY)
    vmem = pl.BlockSpec(memory_space=pltpu.VMEM)
    dma = pltpu.SemaphoreType.DMA
    half = width // 2
    return pl.pallas_call(
        body,
        name="infini",
        out_shape=jax.ShapeDtypeStruct((tokens, width), BF),
        in_specs=[any_space, any_space, any_space, pl.BlockSpec(memory_space=pltpu.SMEM), any_space],
        out_specs=vmem,
        scratch_shapes=[
            pltpu.VMEM((2 * SEG, HD), BF),
            pltpu.VMEM((2 * SEG, 2 * HD), BF),
            pltpu.VMEM((SEG, HD), BF),
            pltpu.VMEM(w_out.shape, BF),
            pltpu.VMEM((HD, 2 * HD), F32),
            pltpu.VMEM((HD + 16, HD), BF),
            pltpu.VMEM((HD + 16, HD), BF),
            pltpu.VMEM((5, HD + 16, HD), BF),
            pltpu.VMEM((HD, 2 * HD), F32),
            pltpu.VMEM((2 * HD, 2 * HD), BF),
            pltpu.VMEM((SEG, HD), F32),
            pltpu.VMEM((SEG, 2 * HD), F32),
            pltpu.VMEM((SEG, HD), BF),
            pltpu.VMEM((ROWS, NB * HD), BF),
            pltpu.VMEM((2, tokens, half), BF),
            pltpu.VMEM((2, tokens, half), BF),
            pltpu.VMEM((4, tokens, half), BF),
            pltpu.VMEM((4, tokens, half), BF),
            pltpu.VMEM((3, tokens, width), BF),
            pltpu.SemaphoreType.REGULAR, pltpu.SemaphoreType.REGULAR((2,)), pltpu.SemaphoreType.REGULAR((3,)),
            dma((3, NB)), dma((3, NB)),
            dma((2, NB)), dma((2, NB)),
            dma((8,)), dma((8,)),
            dma((NB,)), dma((NB,)),
            dma((6,)), dma((6,)),
            dma(()), dma((3,)),
        ],
        compiler_params=pltpu.CompilerParams(
            collective_id=0, has_side_effects=True, vmem_limit_bytes=56 * 1024 * 1024),
    )(queries, keys, values, beta, w_out)


def solution(mesh):
    torus = Mesh(
        mesh.devices.reshape(8, 4, 2, mesh.shape["head"]), ("seq_0", "seq_1", "seq_2", "head")
    )
    return jax.shard_map(
        layer,
        mesh=torus,
        in_specs=(P(SEQ, "head"), P(SEQ, "head"), P(SEQ, "head"), P("head"), P("head", None)),
        out_specs=P(SEQ, "head"),
        check_vma=False,
    )
```

```python
import functools

import jax
import jax.numpy as jnp
from jax import lax
from jax.experimental import pallas as pl
from jax.experimental.pallas import tpu as pltpu
from jax.sharding import Mesh
from jax.sharding import PartitionSpec as P

HD = 128
ROWS = 256
NB = 8
SEG = NB * ROWS
SEQ = ("seq_0", "seq_1", "seq_2")
MESH = pl.DeviceIdType.MESH
BF = jnp.bfloat16
F32 = jnp.float32
SCALE2 = (HD ** -0.5) * 1.4426950408889634
GROUP = 2 * ROWS


def aligned(start, size):
    return start if isinstance(start, int) else pl.multiple_of(start, size)


def rows(block):
    return pl.ds(aligned(block * ROWS, ROWS), ROWS)


def cols(head):
    return pl.ds(aligned(head * HD, HD), HD)


def group_id(block):
    return {"seq_1": block // 2, "seq_2": block % 2}


def phi(x):
    return jnp.where(x > 0, x + 1.0, jnp.exp(jnp.minimum(x, 0.0)))


def body(q_hbm, k_hbm, v_hbm, beta_ref, w_hbm, out_ref,
         kcat, vcat, qh, wv, terms, tmsg, tsum, tin, past, mem, top, acc, att_out, att_in,
         relay_out, relay_in, part_out, part_in, staged,
         go, ok, up, ss, rs, zs, zr, ts, tr, as_, ar, xs, xr, wsem, stage_sem):
    z = lax.axis_index("seq_0")
    y = lax.axis_index("seq_1")
    c = lax.axis_index("seq_2")
    x = lax.axis_index("head")
    place = y * 2 + c
    width = out_ref.shape[1]
    half = width // 2
    quad = lax.rem(z, 4)

    stages = [pltpu.make_async_copy(src, staged.at[i], stage_sem.at[i]) for i, src in enumerate((k_hbm, v_hbm, q_hbm))]
    for copy in stages:
        copy.start()
    pltpu.make_async_copy(w_hbm, wv, wsem).start()

    barrier = pltpu.get_barrier_semaphore()
    for d in range(1, NB):
        other = lax.rem(place + d, NB)

        @pl.when(lax.rem(other, 2) == 0)
        def _():
            pl.semaphore_signal(barrier, 1, device_id=group_id(other), device_id_type=MESH)

    @pl.when(c == 0)
    def _():
        pl.semaphore_wait(barrier, NB - 1)
        pl.semaphore_signal(go, 1, device_id={"seq_2": 1}, device_id_type=MESH)

    @pl.when(c == 1)
    def _():
        pl.semaphore_wait(go, 1)

        @pl.when(z > 0)
        def _():
            pl.semaphore_signal(barrier, 1, device_id={"seq_0": z - 1}, device_id_type=MESH)

        @pl.when(z < 7)
        def _():
            pl.semaphore_signal(barrier, 1, device_id={"seq_0": z + 1}, device_id_type=MESH)

        for d in (1, 3):
            pl.semaphore_signal(barrier, 1, device_id={"head": lax.rem(x + d, 4)}, device_id_type=MESH)

    def pass_word(i):
        pl.semaphore_signal(ok.at[i], 1, device_id={"seq_2": 0}, device_id_type=MESH)

    def hear_of(i):
        @pl.when((c == 1) & (z <= 5 - i))
        def _():
            pl.semaphore_wait(up.at[i], 1)

            if i < 2:
                @pl.when(z > 0)
                def _():
                    pl.semaphore_signal(up.at[i + 1], 1, device_id={"seq_0": z - 1}, device_id_type=MESH)

    own = SEG + place * ROWS
    targets = (
        (staged.at[0], kcat.at[pl.ds(pl.multiple_of(own, ROWS), ROWS), :]),
        (staged.at[1], vcat.at[pl.ds(pl.multiple_of(own, ROWS), ROWS), pl.ds(0, HD)]),
        (staged.at[2], qh.at[rows(place), :]),
    )

    def to_head(t, chip, core):
        block = chip * 2 + core
        return pltpu.make_async_remote_copy(
            src_ref=targets[t][0].at[:, cols(block)], dst_ref=targets[t][1],
            send_sem=ss.at[t, block], recv_sem=rs.at[t, place],
            device_id={"seq_1": chip, "seq_2": core}, device_id_type=MESH)

    others = [(y, 1 - c)]
    for dy in (1, 3, 2):
        for dc in (0, 1):
            others.append((lax.rem(y + dy, 4), lax.rem(c + dc, 2)))
    for t in (0, 1):
        pltpu.make_async_copy((k_hbm, v_hbm)[t].at[:, cols(place)], targets[t][1], rs.at[t, place]).start()
    stages[0].wait()
    stages[1].wait()
    for chip, core in others[:5]:
        for t in (0, 1):
            to_head(t, chip, core).start()
    pltpu.make_async_copy(q_hbm.at[:, cols(place)], targets[2][1], rs.at[2, place]).start()
    stages[2].wait()
    to_head(2, y, 1 - c).start()

    @pl.when(c == 1)
    def _():
        pl.semaphore_wait(barrier, 2 + jnp.where(z < 7, 1, 0) + jnp.where(z > 0, 1, 0))
        pass_word(0)

        @pl.when((z > 0) & (z < 7))
        def _():
            pl.semaphore_signal(up.at[0], 1, device_id={"seq_0": z - 1}, device_id_type=MESH)

    @pl.when(c == 0)
    def _():
        pl.semaphore_wait(ok.at[0], 1)

    vcat[:, HD:] = jnp.ones((2 * SEG, HD), BF)
    terms[...] = jnp.zeros_like(terms)

    code = jnp.where(y == 0, 0 + 3 * 4 + 2 * 16 + 1 * 64,
           jnp.where(y == 1, 1 + 2 * 4 + 3 * 16 + 0 * 64,
           jnp.where(y == 2, 2 + 3 * 4 + 1 * 16 + 0 * 64, 3 + 2 * 4 + 1 * 16 + 0 * 64)))

    def nth(i):
        pair = i // 2
        power = jnp.where(pair == 0, 1, jnp.where(pair == 1, 4, jnp.where(pair == 2, 16, 64)))
        return 2 * lax.rem(code // power, 4) + 1 - lax.rem(i, 2)

    def own_k(p):
        return kcat.at[pl.ds(pl.multiple_of(SEG + p * ROWS, ROWS), ROWS), :]

    def own_v(p):
        return vcat.at[pl.ds(pl.multiple_of(SEG + p * ROWS, ROWS), ROWS), pl.ds(0, HD)]

    def pass_on(t, p):
        src = own_k(p) if t == 0 else own_v(p)
        dst = kcat.at[rows(p), :] if t == 0 else vcat.at[rows(p), pl.ds(0, HD)]
        return pltpu.make_async_remote_copy(
            src_ref=src, dst_ref=dst, send_sem=zs.at[t, p], recv_sem=zr.at[t, p],
            device_id={"seq_0": z + 1}, device_id_type=MESH)

    def arrived(i):
        p = nth(i)
        pltpu.make_async_copy(own_k(p), own_k(p), rs.at[0, p]).wait()
        pltpu.make_async_copy(own_v(p), own_v(p), rs.at[1, p]).wait()
        return p

    def add_terms(p):
        at = pl.ds(pl.multiple_of(SEG + p * ROWS, ROWS), ROWS)
        soft = phi(kcat[at, :].astype(F32)).astype(BF)
        terms[...] += lax.dot_general(soft, vcat[at, :], (((0,), (0,)), ((), ())), preferred_element_type=F32)

    def forward(p):
        @pl.when(z < 7)
        def _():
            pass_on(0, p).start()
            pass_on(1, p).start()

    @pl.loop(0, 2)
    def _(i):
        p = arrived(i)
        forward(p)
        add_terms(p)

    for chip, core in others[5:]:
        for t in (0, 1):
            to_head(t, chip, core).start()
    hear_of(0)

    @pl.loop(2, 4)
    def _(i):
        p = arrived(i)
        forward(p)
        add_terms(p)

    for chip, core in others[1:]:
        to_head(2, chip, core).start()
    hear_of(1)

    @pl.loop(4, NB)
    def _(i):
        add_terms(arrived(i))

    hear_of(2)

    @pl.when(c == 1)
    def _():
        pass_word(1)

    @pl.when(c == 0)
    def _():
        pl.semaphore_wait(ok.at[1], 1)

    def put(dst, block, norm):
        dst[pl.ds(0, HD), :] = block.astype(BF)
        norm_hi = norm.astype(BF)
        norm_lo = (norm - norm_hi.astype(F32)).astype(BF)
        dst[pl.ds(HD, 16), :] = jnp.concatenate([norm_hi, norm_lo], axis=0)

    def add_in(slot):
        pltpu.make_async_copy(tin.at[slot], tin.at[slot], tr.at[slot]).wait()
        past[:, :HD] += tin[slot, pl.ds(0, HD), :].astype(F32)
        n = tin[slot, pl.ds(HD, 16), :].astype(F32)
        past[pl.ds(0, 8), HD:] += n[:8] + n[8:]

    def to_next():
        return pltpu.make_async_remote_copy(
            src_ref=tmsg, dst_ref=tin.at[0], send_sem=ts.at[0], recv_sem=tr.at[0],
            device_id={"seq_0": z + 1}, device_id_type=MESH)

    def to_far(d, slot):
        return pltpu.make_async_remote_copy(
            src_ref=tsum, dst_ref=tin.at[slot], send_sem=ts.at[d], recv_sem=tr.at[slot],
            device_id={"seq_0": z + d}, device_id_type=MESH)

    def put_sum():
        put(tsum, past[:, :HD] + terms[:, :HD], past[pl.ds(0, 8), HD:] + jnp.transpose(terms[:, HD:])[:8])

    norm_rows = jnp.transpose(terms[:, HD:])[:8]
    put(tmsg, terms[:, :HD], norm_rows)
    past[...] = jnp.zeros_like(past)

    @pl.when(lax.rem(z, 2) == 0)
    def _():
        to_next().start()

    forward(nth(4))

    gate = 1.0 / (1.0 + jnp.exp(-jnp.full((8, HD), beta_ref[place], F32)))[0:1]

    def back(j):
        return pltpu.make_async_remote_copy(
            src_ref=att_out.at[rows(j), :], dst_ref=att_in.at[:, cols(place)],
            send_sem=as_.at[j], recv_sem=ar.at[place],
            device_id=group_id(j), device_id_type=MESH)

    row = lax.broadcasted_iota(jnp.int32, (ROWS, ROWS), 0)
    col = lax.broadcasted_iota(jnp.int32, (ROWS, ROWS), 1)

    def at_rows(start):
        return pl.ds(aligned(start, ROWS), ROWS)

    def meet(*jobs):
        held = [None] * len(jobs)

        def score(n):
            j, blocks, first = jobs[n]
            q = qh[rows(j), :]
            old = None if first else top[rows(j), :]
            scores = []
            for start, mask in blocks:
                s = lax.dot_general(q, kcat[at_rows(start), :], (((1,), (1,)), ((), ())), preferred_element_type=F32)
                if mask == "le":
                    s = jnp.where(col <= row, s, -jnp.inf)
                elif mask == "gt":
                    s = jnp.where(col > row, s, -jnp.inf)
                scores.append(s)
            held[n] = (old, scores)

        def soften(n):
            old, scores = held[n]
            peak = functools.reduce(jnp.maximum, [s[:, i * HD:(i + 1) * HD] for s in scores for i in (0, 1)])
            peak = jnp.broadcast_to(jnp.max(peak, axis=1, keepdims=True), (ROWS, HD))
            fade = None
            if old is not None:
                peak = jnp.maximum(old, peak)
                fade = jnp.exp2((old - peak) * SCALE2)
            both = jnp.concatenate([peak, peak], axis=1)
            held[n] = (peak, fade, [jnp.exp2((s - both) * SCALE2).astype(BF) for s in scores])

        def gather(n):
            j, blocks, _ = jobs[n]
            peak, fade, weights = held[n]
            out = None
            for w, (start, _) in zip(weights, blocks):
                more = jnp.dot(w, vcat[at_rows(start), :], preferred_element_type=F32)
                out = more if out is None else out + more
            if fade is not None:
                out = acc[rows(j), :] * jnp.concatenate([fade, fade], axis=1) + out
            acc[rows(j), :] = out
            held[n] = peak

        for n in range(len(jobs) + 2):
            if n < len(jobs):
                score(n)
            if 0 <= n - 1 < len(jobs):
                soften(n - 1)
            if n >= 2:
                gather(n - 2)
        for (j, _, _), peak in zip(jobs, held):
            top[rows(j), :] = peak

    def whole(g, base):
        return [(2 * g + i, [(base, None), (base + ROWS, None)], False) for i in (0, 1)]

    def previous_diagonal(g):
        base = g * GROUP
        return [(2 * g, [(base, "gt"), (base + ROWS, None)], False), (2 * g + 1, [(base + ROWS, "gt")], False)]

    near = jnp.where(y == 0, 0 + 3 * 4 + 1 * 16 + 2 * 64,
           jnp.where(y == 1, 1 + 2 * 4 + 0 * 16 + 3 * 64,
           jnp.where(y == 2, 2 + 3 * 4 + 1 * 16 + 0 * 64, 3 + 2 * 4 + 0 * 16 + 1 * 64)))

    @pl.loop(0, 4)
    def _(i):
        power = jnp.where(i == 0, 1, jnp.where(i == 1, 4, jnp.where(i == 2, 16, 64)))
        g = lax.rem(near // power, 4)
        for j in (2 * g, 2 * g + 1):
            pltpu.make_async_copy(qh.at[rows(j), :], qh.at[rows(j), :], rs.at[2, j]).wait()
        for own_g in range(4):
            @pl.when(g == own_g)
            def _():
                meet(*[(j, [(SEG + k * ROWS, None) for k in range(j)] + [(SEG + j * ROWS, "le")], True)
                       for j in (2 * own_g, 2 * own_g + 1)])

        @pl.when(i == 1)
        def _():
            @pl.when(quad == 1)
            def _():
                add_in(0)
                put_sum()
                for d in (1, 2):
                    to_far(d, 1).start()

            forward(nth(5))

            @pl.when(z != 3)
            def _():
                forward(nth(6))

        @pl.when(i == 3)
        def _():
            @pl.when(z == 3)
            def _():
                add_in(0)
                add_in(1)
                put_sum()
                for d in (1, 2, 3, 4):
                    to_far(d, 2).start()
                forward(nth(6))

            forward(nth(7))

    def finish(j):
        local = acc[rows(j), :HD] / acc[rows(j), HD:]
        soft = phi(qh[rows(j), :].astype(F32)).astype(BF)
        found = jnp.dot(jnp.concatenate([soft, soft], axis=1), mem[...], preferred_element_type=F32)
        from_memory = found[:, :HD] / (1.0 + found[:, HD:])
        att_out[rows(j), :] = (gate * from_memory + (1.0 - gate) * local).astype(BF)

        @pl.when(j != place)
        def _():
            back(j).start()

        @pl.when(j == place)
        def _():
            pltpu.make_async_copy(att_out.at[rows(j), :], att_in.at[:, cols(place)], ar.at[place]).start()

    def came(j):
        pltpu.make_async_copy(kcat.at[rows(j), :], kcat.at[rows(j), :], zr.at[0, j]).wait()
        pltpu.make_async_copy(vcat.at[rows(j), pl.ds(0, HD)], vcat.at[rows(j), pl.ds(0, HD)], zr.at[1, j]).wait()

    def meet_previous(g):
        @pl.when(z > 0)
        def _():
            came(2 * g + 1)
            came(2 * g)
            jobs = previous_diagonal(g)
            for k in range(g):
                jobs = jobs + whole(k, g * GROUP)
            meet(*jobs)

    meet_previous(3)
    meet_previous(2)

    @pl.when(z == 7)
    def _():
        add_in(0)

    @pl.when((quad == 2) | (z == 7))
    def _():
        add_in(1)

    @pl.when(z > 3)
    def _():
        add_in(2)

    norm_cols = jnp.transpose(jnp.broadcast_to(past[0:1, HD:], (HD, HD)))
    full = jnp.concatenate([past[:, :HD], norm_cols], axis=1)
    full_hi = full.astype(BF)
    mem[pl.ds(0, HD), :] = full_hi
    mem[pl.ds(HD, HD), :] = (full - full_hi.astype(F32)).astype(BF)

    @pl.loop(0, 4)
    def _(i):
        finish(7 - i)

    @pl.when(y == 0)
    def _():
        meet_previous(0)
        meet_previous(1)

        @pl.loop(0, 4)
        def _(j):
            finish(j)

    @pl.when(y != 0)
    def _():
        meet_previous(1)

        @pl.loop(2, 4)
        def _(j):
            finish(j)

        @pl.when(z > 0)
        def _():
            came(1)
            meet((1, [(ROWS, "gt")], False), (0, [(ROWS, None)], False))

        finish(1)

        @pl.when(z > 0)
        def _():
            came(0)
            meet((0, [(0, "gt")], False))

        finish(0)

    @pl.loop(0, NB)
    def _(h):
        pltpu.make_async_copy(att_in.at[:, cols(h)], att_in.at[:, cols(h)], ar.at[h]).wait()

    pltpu.make_async_copy(w_hbm, wv, wsem).wait()

    up, down, far = lax.rem(x + 1, 4), lax.rem(x + 3, 4), lax.rem(x + 2, 4)

    def product(owner, start, size):
        at = pl.ds(pl.multiple_of(owner * width + start, HD), size)
        return jnp.dot(att_in[...], wv[:, at], preferred_element_type=F32)

    def to_x(src, dst, i, target):
        return pltpu.make_async_remote_copy(
            src_ref=src, dst_ref=dst, send_sem=xs.at[i], recv_sem=xr.at[i],
            device_id={"head": target}, device_id_type=MESH)

    copies = []

    def send(src, dst, i, target):
        copy = to_x(src, dst, i, target)
        copy.start()
        copies.append(copy)

    relay_out[0] = product(far, 0, half).astype(BF)
    send(relay_out.at[0], relay_in.at[0], 0, up)
    relay_out[1] = product(far, half, half).astype(BF)
    send(relay_out.at[1], relay_in.at[1], 1, down)
    part_out[1] = product(up, half, half).astype(BF)
    send(part_out.at[1], part_in.at[1], 2, up)
    part_out[2] = product(down, 0, half).astype(BF)
    send(part_out.at[2], part_in.at[2], 3, down)
    first = product(up, 0, half)
    copies[0].wait_recv()
    part_out[0] = (first + relay_in[0].astype(F32)).astype(BF)
    send(part_out.at[0], part_in.at[0], 4, up)
    second = product(down, half, half)
    copies[1].wait_recv()
    part_out[3] = (second + relay_in[1].astype(F32)).astype(BF)
    send(part_out.at[3], part_in.at[3], 5, down)
    left = product(x, 0, half)
    right = product(x, half, half)
    copies[2].wait_recv()
    copies[3].wait_recv()
    left = left + part_in[2].astype(F32)
    right = right + part_in[1].astype(F32)
    copies[4].wait_recv()
    out_ref[:, :half] = (left + part_in[0].astype(F32)).astype(BF)
    copies[5].wait_recv()
    out_ref[:, half:] = (right + part_in[3].astype(F32)).astype(BF)

    for copy in copies:
        copy.wait_send()
    for t in range(3):
        for chip, core in others:
            to_head(t, chip, core).wait_send()

    @pl.loop(0, NB)
    def _(p):
        @pl.when(z < 7)
        def _():
            pass_on(0, p).wait_send()
            pass_on(1, p).wait_send()

        @pl.when(p != place)
        def _():
            back(p).wait_send()

    @pl.when(lax.rem(z, 2) == 0)
    def _():
        to_next().wait_send()

    @pl.when(quad == 1)
    def _():
        for d in (1, 2):
            to_far(d, 1).wait_send()

    @pl.when(z == 3)
    def _():
        for d in (1, 2, 3, 4):
            to_far(d, 2).wait_send()


def layer(queries, keys, values, beta, w_out):
    tokens, width = queries.shape
    any_space = pl.BlockSpec(memory_space=pl.ANY)
    vmem = pl.BlockSpec(memory_space=pltpu.VMEM)
    dma = pltpu.SemaphoreType.DMA
    half = width // 2
    return pl.pallas_call(
        body,
        name="infini",
        out_shape=jax.ShapeDtypeStruct((tokens, width), BF),
        in_specs=[any_space, any_space, any_space, pl.BlockSpec(memory_space=pltpu.SMEM), any_space],
        out_specs=vmem,
        scratch_shapes=[
            pltpu.VMEM((2 * SEG, HD), BF),
            pltpu.VMEM((2 * SEG, 2 * HD), BF),
            pltpu.VMEM((SEG, HD), BF),
            pltpu.VMEM(w_out.shape, BF),
            pltpu.VMEM((HD, 2 * HD), F32),
            pltpu.VMEM((HD + 16, HD), BF),
            pltpu.VMEM((HD + 16, HD), BF),
            pltpu.VMEM((5, HD + 16, HD), BF),
            pltpu.VMEM((HD, 2 * HD), F32),
            pltpu.VMEM((2 * HD, 2 * HD), BF),
            pltpu.VMEM((SEG, HD), F32),
            pltpu.VMEM((SEG, 2 * HD), F32),
            pltpu.VMEM((SEG, HD), BF),
            pltpu.VMEM((ROWS, NB * HD), BF),
            pltpu.VMEM((2, tokens, half), BF),
            pltpu.VMEM((2, tokens, half), BF),
            pltpu.VMEM((4, tokens, half), BF),
            pltpu.VMEM((4, tokens, half), BF),
            pltpu.VMEM((3, tokens, width), BF),
            pltpu.SemaphoreType.REGULAR, pltpu.SemaphoreType.REGULAR((2,)), pltpu.SemaphoreType.REGULAR((3,)),
            dma((3, NB)), dma((3, NB)),
            dma((2, NB)), dma((2, NB)),
            dma((8,)), dma((8,)),
            dma((NB,)), dma((NB,)),
            dma((6,)), dma((6,)),
            dma(()), dma((3,)),
        ],
        compiler_params=pltpu.CompilerParams(
            collective_id=0, has_side_effects=True, vmem_limit_bytes=56 * 1024 * 1024),
    )(queries, keys, values, beta, w_out)


def solution(mesh):
    torus = Mesh(
        mesh.devices.reshape(8, 4, 2, mesh.shape["head"]), ("seq_0", "seq_1", "seq_2", "head")
    )
    return jax.shard_map(
        layer,
        mesh=torus,
        in_specs=(P(SEQ, "head"), P(SEQ, "head"), P(SEQ, "head"), P("head"), P("head", None)),
        out_specs=P(SEQ, "head"),
        check_vma=False,
    )
```

```python
import functools

import jax
import jax.numpy as jnp
from jax import lax
from jax.experimental import pallas as pl
from jax.experimental.pallas import tpu as pltpu
from jax.sharding import Mesh
from jax.sharding import PartitionSpec as P

HD = 128
ROWS = 256
NB = 8
SEG = NB * ROWS
SEQ = ("seq_0", "seq_1", "seq_2")
MESH = pl.DeviceIdType.MESH
BF = jnp.bfloat16
F32 = jnp.float32
SCALE2 = (HD ** -0.5) * 1.4426950408889634
GROUP = 2 * ROWS


def aligned(start, size):
    return start if isinstance(start, int) else pl.multiple_of(start, size)


def rows(block):
    return pl.ds(aligned(block * ROWS, ROWS), ROWS)


def cols(head):
    return pl.ds(aligned(head * HD, HD), HD)


def group_id(block):
    return {"seq_1": block // 2, "seq_2": block % 2}


def phi(x):
    return jnp.where(x > 0, x + 1.0, jnp.exp(jnp.minimum(x, 0.0)))


def body(q_hbm, k_hbm, v_hbm, beta_ref, w_hbm, out_ref,
         kcat, vcat, qh, wv, terms, tmsg, tsum, tin, past, mem, top, acc, att_out, att_in,
         relay_out, relay_in, part_out, part_in, staged,
         go, ok, up, ss, rs, zs, zr, ts, tr, as_, ar, xs, xr, wsem, stage_sem):
    z = lax.axis_index("seq_0")
    y = lax.axis_index("seq_1")
    c = lax.axis_index("seq_2")
    x = lax.axis_index("head")
    place = y * 2 + c
    width = out_ref.shape[1]
    half = width // 2
    quad = lax.rem(z, 4)

    stages = [pltpu.make_async_copy(src, staged.at[i], stage_sem.at[i]) for i, src in enumerate((k_hbm, v_hbm, q_hbm))]
    for copy in stages:
        copy.start()
    pltpu.make_async_copy(w_hbm, wv, wsem).start()

    barrier = pltpu.get_barrier_semaphore()
    for d in range(1, NB):
        other = lax.rem(place + d, NB)

        @pl.when(lax.rem(other, 2) == 0)
        def _():
            pl.semaphore_signal(barrier, 1, device_id=group_id(other), device_id_type=MESH)

    @pl.when(c == 0)
    def _():
        pl.semaphore_wait(barrier, NB - 1)
        pl.semaphore_signal(go, 1, device_id={"seq_2": 1}, device_id_type=MESH)

    @pl.when(c == 1)
    def _():
        pl.semaphore_wait(go, 1)

        @pl.when(z > 0)
        def _():
            pl.semaphore_signal(barrier, 1, device_id={"seq_0": z - 1}, device_id_type=MESH)

        @pl.when(z < 7)
        def _():
            pl.semaphore_signal(barrier, 1, device_id={"seq_0": z + 1}, device_id_type=MESH)

        for d in (1, 3):
            pl.semaphore_signal(barrier, 1, device_id={"head": lax.rem(x + d, 4)}, device_id_type=MESH)

    def pass_word(i):
        pl.semaphore_signal(ok.at[i], 1, device_id={"seq_2": 0}, device_id_type=MESH)

    def hear_of(i):
        @pl.when((c == 1) & (z <= 5 - i))
        def _():
            pl.semaphore_wait(up.at[i], 1)

            if i < 2:
                @pl.when(z > 0)
                def _():
                    pl.semaphore_signal(up.at[i + 1], 1, device_id={"seq_0": z - 1}, device_id_type=MESH)

    own = SEG + place * ROWS
    targets = (
        (staged.at[0], kcat.at[pl.ds(pl.multiple_of(own, ROWS), ROWS), :]),
        (staged.at[1], vcat.at[pl.ds(pl.multiple_of(own, ROWS), ROWS), pl.ds(0, HD)]),
        (staged.at[2], qh.at[rows(place), :]),
    )

    def to_head(t, chip, core):
        block = chip * 2 + core
        return pltpu.make_async_remote_copy(
            src_ref=targets[t][0].at[:, cols(block)], dst_ref=targets[t][1],
            send_sem=ss.at[t, block], recv_sem=rs.at[t, place],
            device_id={"seq_1": chip, "seq_2": core}, device_id_type=MESH)

    others = [(y, 1 - c)]
    for dy in (1, 3, 2):
        for dc in (0, 1):
            others.append((lax.rem(y + dy, 4), lax.rem(c + dc, 2)))
    for t in (0, 1):
        pltpu.make_async_copy((k_hbm, v_hbm)[t].at[:, cols(place)], targets[t][1], rs.at[t, place]).start()
    stages[0].wait()
    stages[1].wait()
    for chip, core in others[:5]:
        for t in (0, 1):
            to_head(t, chip, core).start()
    pltpu.make_async_copy(q_hbm.at[:, cols(place)], targets[2][1], rs.at[2, place]).start()
    stages[2].wait()
    to_head(2, y, 1 - c).start()

    @pl.when(c == 1)
    def _():
        pl.semaphore_wait(barrier, 2 + jnp.where(z < 7, 1, 0) + jnp.where(z > 0, 1, 0))
        pass_word(0)

        @pl.when((z > 0) & (z < 7))
        def _():
            pl.semaphore_signal(up.at[0], 1, device_id={"seq_0": z - 1}, device_id_type=MESH)

    @pl.when(c == 0)
    def _():
        pl.semaphore_wait(ok.at[0], 1)

    vcat[:, HD:] = jnp.ones((2 * SEG, HD), BF)
    terms[...] = jnp.zeros_like(terms)

    code = jnp.where(y == 0, 0 + 3 * 4 + 2 * 16 + 1 * 64,
           jnp.where(y == 1, 1 + 2 * 4 + 3 * 16 + 0 * 64,
           jnp.where(y == 2, 2 + 3 * 4 + 1 * 16 + 0 * 64, 3 + 2 * 4 + 1 * 16 + 0 * 64)))

    def nth(i):
        pair = i // 2
        power = jnp.where(pair == 0, 1, jnp.where(pair == 1, 4, jnp.where(pair == 2, 16, 64)))
        return 2 * lax.rem(code // power, 4) + 1 - lax.rem(i, 2)

    def own_k(p):
        return kcat.at[pl.ds(pl.multiple_of(SEG + p * ROWS, ROWS), ROWS), :]

    def own_v(p):
        return vcat.at[pl.ds(pl.multiple_of(SEG + p * ROWS, ROWS), ROWS), pl.ds(0, HD)]

    def pass_on(t, p):
        src = own_k(p) if t == 0 else own_v(p)
        dst = kcat.at[rows(p), :] if t == 0 else vcat.at[rows(p), pl.ds(0, HD)]
        return pltpu.make_async_remote_copy(
            src_ref=src, dst_ref=dst, send_sem=zs.at[t, p], recv_sem=zr.at[t, p],
            device_id={"seq_0": z + 1}, device_id_type=MESH)

    def arrived(i):
        p = nth(i)
        pltpu.make_async_copy(own_k(p), own_k(p), rs.at[0, p]).wait()
        pltpu.make_async_copy(own_v(p), own_v(p), rs.at[1, p]).wait()
        return p

    def add_terms(p):
        at = pl.ds(pl.multiple_of(SEG + p * ROWS, ROWS), ROWS)
        soft = phi(kcat[at, :].astype(F32)).astype(BF)
        terms[...] += lax.dot_general(soft, vcat[at, :], (((0,), (0,)), ((), ())), preferred_element_type=F32)

    def forward(p):
        @pl.when(z < 7)
        def _():
            pass_on(0, p).start()
            pass_on(1, p).start()

    @pl.loop(0, 2)
    def _(i):
        p = arrived(i)
        forward(p)
        add_terms(p)

    for chip, core in others[5:]:
        for t in (0, 1):
            to_head(t, chip, core).start()
    hear_of(0)

    @pl.loop(2, 4)
    def _(i):
        p = arrived(i)
        forward(p)
        add_terms(p)

    for chip, core in others[1:]:
        to_head(2, chip, core).start()
    hear_of(1)

    @pl.loop(4, NB)
    def _(i):
        add_terms(arrived(i))

    hear_of(2)

    @pl.when(c == 1)
    def _():
        pass_word(1)

    @pl.when(c == 0)
    def _():
        pl.semaphore_wait(ok.at[1], 1)

    def put(dst, block, norm):
        dst[pl.ds(0, HD), :] = block.astype(BF)
        norm_hi = norm.astype(BF)
        norm_lo = (norm - norm_hi.astype(F32)).astype(BF)
        dst[pl.ds(HD, 16), :] = jnp.concatenate([norm_hi, norm_lo], axis=0)

    def add_in(slot):
        pltpu.make_async_copy(tin.at[slot], tin.at[slot], tr.at[slot]).wait()
        past[:, :HD] += tin[slot, pl.ds(0, HD), :].astype(F32)
        n = tin[slot, pl.ds(HD, 16), :].astype(F32)
        past[pl.ds(0, 8), HD:] += n[:8] + n[8:]

    def to_next():
        return pltpu.make_async_remote_copy(
            src_ref=tmsg, dst_ref=tin.at[0], send_sem=ts.at[0], recv_sem=tr.at[0],
            device_id={"seq_0": z + 1}, device_id_type=MESH)

    def to_far(d, slot):
        return pltpu.make_async_remote_copy(
            src_ref=tsum, dst_ref=tin.at[slot], send_sem=ts.at[d], recv_sem=tr.at[slot],
            device_id={"seq_0": z + d}, device_id_type=MESH)

    def put_sum():
        put(tsum, past[:, :HD] + terms[:, :HD], past[pl.ds(0, 8), HD:] + jnp.transpose(terms[:, HD:])[:8])

    norm_rows = jnp.transpose(terms[:, HD:])[:8]
    put(tmsg, terms[:, :HD], norm_rows)
    past[...] = jnp.zeros_like(past)

    @pl.when(lax.rem(z, 2) == 0)
    def _():
        to_next().start()

    forward(nth(4))

    @pl.when(quad != 1)
    def _():
        forward(nth(5))

    gate = 1.0 / (1.0 + jnp.exp(-jnp.full((8, HD), beta_ref[place], F32)))[0:1]

    def back(j):
        return pltpu.make_async_remote_copy(
            src_ref=att_out.at[rows(j), :], dst_ref=att_in.at[:, cols(place)],
            send_sem=as_.at[j], recv_sem=ar.at[place],
            device_id=group_id(j), device_id_type=MESH)

    row = lax.broadcasted_iota(jnp.int32, (ROWS, ROWS), 0)
    col = lax.broadcasted_iota(jnp.int32, (ROWS, ROWS), 1)

    def at_rows(start):
        return pl.ds(aligned(start, ROWS), ROWS)

    def meet(*jobs):
        held = [None] * len(jobs)

        def score(n):
            j, blocks, first = jobs[n]
            q = qh[rows(j), :]
            old = None if first else top[rows(j), :]
            scores = []
            for start, mask in blocks:
                s = lax.dot_general(q, kcat[at_rows(start), :], (((1,), (1,)), ((), ())), preferred_element_type=F32)
                if mask == "le":
                    s = jnp.where(col <= row, s, -jnp.inf)
                elif mask == "gt":
                    s = jnp.where(col > row, s, -jnp.inf)
                scores.append(s)
            held[n] = (old, scores)

        def soften(n):
            old, scores = held[n]
            peak = functools.reduce(jnp.maximum, [s[:, i * HD:(i + 1) * HD] for s in scores for i in (0, 1)])
            peak = jnp.broadcast_to(jnp.max(peak, axis=1, keepdims=True), (ROWS, HD))
            fade = None
            if old is not None:
                peak = jnp.maximum(old, peak)
                fade = jnp.exp2((old - peak) * SCALE2)
            both = jnp.concatenate([peak, peak], axis=1)
            held[n] = (peak, fade, [jnp.exp2((s - both) * SCALE2).astype(BF) for s in scores])

        def gather(n):
            j, blocks, _ = jobs[n]
            peak, fade, weights = held[n]
            out = None
            for w, (start, _) in zip(weights, blocks):
                more = jnp.dot(w, vcat[at_rows(start), :], preferred_element_type=F32)
                out = more if out is None else out + more
            if fade is not None:
                out = acc[rows(j), :] * jnp.concatenate([fade, fade], axis=1) + out
            acc[rows(j), :] = out
            held[n] = peak

        for n in range(len(jobs) + 2):
            if n < len(jobs):
                score(n)
            if 0 <= n - 1 < len(jobs):
                soften(n - 1)
            if n >= 2:
                gather(n - 2)
        for (j, _, _), peak in zip(jobs, held):
            top[rows(j), :] = peak

    def whole(g, base):
        return [(2 * g + i, [(base, None), (base + ROWS, None)], False) for i in (0, 1)]

    def previous_diagonal(g):
        base = g * GROUP
        return [(2 * g, [(base, "gt"), (base + ROWS, None)], False), (2 * g + 1, [(base + ROWS, "gt")], False)]

    near = jnp.where(y == 0, 0 + 3 * 4 + 1 * 16 + 2 * 64,
           jnp.where(y == 1, 1 + 2 * 4 + 0 * 16 + 3 * 64,
           jnp.where(y == 2, 2 + 3 * 4 + 1 * 16 + 0 * 64, 3 + 2 * 4 + 0 * 16 + 1 * 64)))

    @pl.loop(0, 4)
    def _(i):
        power = jnp.where(i == 0, 1, jnp.where(i == 1, 4, jnp.where(i == 2, 16, 64)))
        g = lax.rem(near // power, 4)
        for j in (2 * g, 2 * g + 1):
            pltpu.make_async_copy(qh.at[rows(j), :], qh.at[rows(j), :], rs.at[2, j]).wait()
        for own_g in range(4):
            @pl.when(g == own_g)
            def _():
                meet(*[(j, [(SEG + k * ROWS, None) for k in range(j)] + [(SEG + j * ROWS, "le")], True)
                       for j in (2 * own_g, 2 * own_g + 1)])

        @pl.when(i == 1)
        def _():
            @pl.when(quad == 1)
            def _():
                add_in(0)
                put_sum()
                for d in (1, 2):
                    to_far(d, 1).start()
                forward(nth(5))

            @pl.when(z != 3)
            def _():
                forward(nth(6))

        @pl.when(i == 3)
        def _():
            @pl.when(z == 3)
            def _():
                add_in(0)
                add_in(1)
                put_sum()
                for d in (1, 2, 3, 4):
                    to_far(d, 2).start()
                forward(nth(6))

            forward(nth(7))

    def finish(j):
        local = acc[rows(j), :HD] / acc[rows(j), HD:]
        soft = phi(qh[rows(j), :].astype(F32)).astype(BF)
        found = jnp.dot(jnp.concatenate([soft, soft], axis=1), mem[...], preferred_element_type=F32)
        from_memory = found[:, :HD] / (1.0 + found[:, HD:])
        att_out[rows(j), :] = (gate * from_memory + (1.0 - gate) * local).astype(BF)

        @pl.when(j != place)
        def _():
            back(j).start()

        @pl.when(j == place)
        def _():
            pltpu.make_async_copy(att_out.at[rows(j), :], att_in.at[:, cols(place)], ar.at[place]).start()

    def came(j):
        pltpu.make_async_copy(kcat.at[rows(j), :], kcat.at[rows(j), :], zr.at[0, j]).wait()
        pltpu.make_async_copy(vcat.at[rows(j), pl.ds(0, HD)], vcat.at[rows(j), pl.ds(0, HD)], zr.at[1, j]).wait()

    def meet_previous(g):
        @pl.when(z > 0)
        def _():
            came(2 * g + 1)
            came(2 * g)
            jobs = previous_diagonal(g)
            for k in range(g):
                jobs = jobs + whole(k, g * GROUP)
            meet(*jobs)

    meet_previous(3)
    meet_previous(2)

    @pl.when(z == 7)
    def _():
        add_in(0)

    @pl.when((quad == 2) | (z == 7))
    def _():
        add_in(1)

    @pl.when(z > 3)
    def _():
        add_in(2)

    norm_cols = jnp.transpose(jnp.broadcast_to(past[0:1, HD:], (HD, HD)))
    full = jnp.concatenate([past[:, :HD], norm_cols], axis=1)
    full_hi = full.astype(BF)
    mem[pl.ds(0, HD), :] = full_hi
    mem[pl.ds(HD, HD), :] = (full - full_hi.astype(F32)).astype(BF)

    @pl.loop(0, 4)
    def _(i):
        finish(7 - i)

    @pl.when(y == 0)
    def _():
        meet_previous(0)
        meet_previous(1)

        @pl.loop(0, 4)
        def _(j):
            finish(j)

    @pl.when(y != 0)
    def _():
        meet_previous(1)

        @pl.loop(2, 4)
        def _(j):
            finish(j)

        @pl.when(z > 0)
        def _():
            came(1)
            meet((1, [(ROWS, "gt")], False), (0, [(ROWS, None)], False))

        finish(1)

        @pl.when(z > 0)
        def _():
            came(0)
            meet((0, [(0, "gt")], False))

        finish(0)

    @pl.loop(0, NB)
    def _(h):
        pltpu.make_async_copy(att_in.at[:, cols(h)], att_in.at[:, cols(h)], ar.at[h]).wait()

    pltpu.make_async_copy(w_hbm, wv, wsem).wait()

    up, down, far = lax.rem(x + 1, 4), lax.rem(x + 3, 4), lax.rem(x + 2, 4)

    def product(owner, start, size):
        at = pl.ds(pl.multiple_of(owner * width + start, HD), size)
        return jnp.dot(att_in[...], wv[:, at], preferred_element_type=F32)

    def to_x(src, dst, i, target):
        return pltpu.make_async_remote_copy(
            src_ref=src, dst_ref=dst, send_sem=xs.at[i], recv_sem=xr.at[i],
            device_id={"head": target}, device_id_type=MESH)

    copies = []

    def send(src, dst, i, target):
        copy = to_x(src, dst, i, target)
        copy.start()
        copies.append(copy)

    relay_out[0] = product(far, 0, half).astype(BF)
    send(relay_out.at[0], relay_in.at[0], 0, up)
    relay_out[1] = product(far, half, half).astype(BF)
    send(relay_out.at[1], relay_in.at[1], 1, down)
    part_out[1] = product(up, half, half).astype(BF)
    send(part_out.at[1], part_in.at[1], 2, up)
    part_out[2] = product(down, 0, half).astype(BF)
    send(part_out.at[2], part_in.at[2], 3, down)
    first = product(up, 0, half)
    copies[0].wait_recv()
    part_out[0] = (first + relay_in[0].astype(F32)).astype(BF)
    send(part_out.at[0], part_in.at[0], 4, up)
    second = product(down, half, half)
    copies[1].wait_recv()
    part_out[3] = (second + relay_in[1].astype(F32)).astype(BF)
    send(part_out.at[3], part_in.at[3], 5, down)
    left = product(x, 0, half)
    right = product(x, half, half)
    copies[2].wait_recv()
    copies[3].wait_recv()
    left = left + part_in[2].astype(F32)
    right = right + part_in[1].astype(F32)
    copies[4].wait_recv()
    out_ref[:, :half] = (left + part_in[0].astype(F32)).astype(BF)
    copies[5].wait_recv()
    out_ref[:, half:] = (right + part_in[3].astype(F32)).astype(BF)

    for copy in copies:
        copy.wait_send()
    for t in range(3):
        for chip, core in others:
            to_head(t, chip, core).wait_send()

    @pl.loop(0, NB)
    def _(p):
        @pl.when(z < 7)
        def _():
            pass_on(0, p).wait_send()
            pass_on(1, p).wait_send()

        @pl.when(p != place)
        def _():
            back(p).wait_send()

    @pl.when(lax.rem(z, 2) == 0)
    def _():
        to_next().wait_send()

    @pl.when(quad == 1)
    def _():
        for d in (1, 2):
            to_far(d, 1).wait_send()

    @pl.when(z == 3)
    def _():
        for d in (1, 2, 3, 4):
            to_far(d, 2).wait_send()


def layer(queries, keys, values, beta, w_out):
    tokens, width = queries.shape
    any_space = pl.BlockSpec(memory_space=pl.ANY)
    vmem = pl.BlockSpec(memory_space=pltpu.VMEM)
    dma = pltpu.SemaphoreType.DMA
    half = width // 2
    return pl.pallas_call(
        body,
        name="infini",
        out_shape=jax.ShapeDtypeStruct((tokens, width), BF),
        in_specs=[any_space, any_space, any_space, pl.BlockSpec(memory_space=pltpu.SMEM), any_space],
        out_specs=vmem,
        scratch_shapes=[
            pltpu.VMEM((2 * SEG, HD), BF),
            pltpu.VMEM((2 * SEG, 2 * HD), BF),
            pltpu.VMEM((SEG, HD), BF),
            pltpu.VMEM(w_out.shape, BF),
            pltpu.VMEM((HD, 2 * HD), F32),
            pltpu.VMEM((HD + 16, HD), BF),
            pltpu.VMEM((HD + 16, HD), BF),
            pltpu.VMEM((5, HD + 16, HD), BF),
            pltpu.VMEM((HD, 2 * HD), F32),
            pltpu.VMEM((2 * HD, 2 * HD), BF),
            pltpu.VMEM((SEG, HD), F32),
            pltpu.VMEM((SEG, 2 * HD), F32),
            pltpu.VMEM((SEG, HD), BF),
            pltpu.VMEM((ROWS, NB * HD), BF),
            pltpu.VMEM((2, tokens, half), BF),
            pltpu.VMEM((2, tokens, half), BF),
            pltpu.VMEM((4, tokens, half), BF),
            pltpu.VMEM((4, tokens, half), BF),
            pltpu.VMEM((3, tokens, width), BF),
            pltpu.SemaphoreType.REGULAR, pltpu.SemaphoreType.REGULAR((2,)), pltpu.SemaphoreType.REGULAR((3,)),
            dma((3, NB)), dma((3, NB)),
            dma((2, NB)), dma((2, NB)),
            dma((8,)), dma((8,)),
            dma((NB,)), dma((NB,)),
            dma((6,)), dma((6,)),
            dma(()), dma((3,)),
        ],
        compiler_params=pltpu.CompilerParams(
            collective_id=0, has_side_effects=True, vmem_limit_bytes=56 * 1024 * 1024),
    )(queries, keys, values, beta, w_out)


def solution(mesh):
    torus = Mesh(
        mesh.devices.reshape(8, 4, 2, mesh.shape["head"]), ("seq_0", "seq_1", "seq_2", "head")
    )
    return jax.shard_map(
        layer,
        mesh=torus,
        in_specs=(P(SEQ, "head"), P(SEQ, "head"), P(SEQ, "head"), P("head"), P("head", None)),
        out_specs=P(SEQ, "head"),
        check_vma=False,
    )
```
